256 devices in a mesh: seq: 64 (over x, z, core), tp: 4 (over y).
Axes of the slice: x: 4, y: 4, z: 8, core: 2. Of those that a mesh axis runs over, the one named last changes fastest.
Arguments:
- layer_in: bfloat16 [49152, 2048], P('seq', 'tp'), may hold values from -6 to 6
- attn_gain: float32 [2048], replicated, may hold values from 0.1 to 1.9
- qkv_weight: bfloat16 [3, 2048, 1024], P(None, None, 'tp'), may hold values from -0.125 to 0.125
- log_decay: float32 [8, 49152], P('tp', 'seq'), may hold values from -0.1 to 0
- write_rate: float32 [8, 49152], P('tp', 'seq'), may hold values from 0 to 0.9
- head_gain: float32 [128], replicated, may hold values from 0.1 to 1.9
- out_weight: bfloat16 [1024, 2048], P('tp'), may hold values from -0.1875 to 0.1875
- ffn_gain: float32 [2048], replicated, may hold values from 0.1 to 1.9
- gate_weight: bfloat16 [2048, 2560], P(None, 'tp'), may hold values from -0.125 to 0.125
- up_weight: bfloat16 [2048, 2560], P(None, 'tp'), may hold values from -0.125 to 0.125
- down_weight: bfloat16 [2560, 2048], P('tp'), may hold values from -0.125 to 0.125
Outputs:
- layer_out: bfloat16 [49152, 2048], P('seq', 'tp')
The draws below stay inside these ranges and needn't reach their ends.
All inputs are finite; a program needn't handle non-finite values.
Results may differ from the reference program's by a relative error of at most 0.014.
Values may be sent and summed in bfloat16 or wider, within the bound.
A program may use at most 128 MiB of HBM per device.

```python
import math
import jax
import jax.numpy as jnp
from jax import lax

D = 2048
HEADS = 8
DK = 128
FF = 2560
TOK_DEV = 768
SEQLEN = 49152
N_TP = 4


def head_kinds(key):
    kind_key = jax.random.fold_in(key, 101)
    order_key = jax.random.fold_in(key, 102)
    slow_share = 0.5
    slow_heads = jax.random.uniform(kind_key, (HEADS,)) < slow_share
    order = jax.random.permutation(order_key, HEADS)
    slow_heads = slow_heads.at[order[0]].set(True)
    slow_heads = slow_heads.at[order[1]].set(False)
    return slow_heads


def draw_log_decay(key, part):
    slow_heads = head_kinds(key)
    slow_rate = jax.random.uniform(jax.random.fold_in(key, 1), (HEADS, 1), minval=0.2, maxval=0.6) / SEQLEN
    fast_rate = jax.random.uniform(jax.random.fold_in(key, 2), (HEADS, 1), minval=1.0 / 50.0, maxval=1.0 / 30.0)
    base_rate = jnp.where(slow_heads[:, None], slow_rate, fast_rate)
    blocks = SEQLEN // TOK_DEV
    device_scale = jnp.exp(jax.random.uniform(jax.random.fold_in(key, 3), (HEADS, blocks, 1), minval=math.log(0.5), maxval=math.log(2.0)))
    device_scale = jnp.broadcast_to(device_scale, (HEADS, blocks, TOK_DEV)).reshape(HEADS, SEQLEN)
    jitter = jax.random.uniform(jax.random.fold_in(key, 4), (HEADS, SEQLEN), minval=0.5, maxval=1.5)
    return -(base_rate * device_scale * jitter).astype(jnp.float32)


def draw_write_rate(key, part):
    slow_heads = head_kinds(key)
    slow_rate = jax.random.uniform(jax.random.fold_in(key, 5), (HEADS, SEQLEN), minval=0.05, maxval=0.4) * DK / SEQLEN
    fast_rate = jax.random.uniform(jax.random.fold_in(key, 6), (HEADS, SEQLEN), minval=0.1, maxval=0.9)
    chosen = jnp.where(slow_heads[:, None], slow_rate, fast_rate)
    return jnp.minimum(chosen, 0.9).astype(jnp.float32)


def level_of(rng, extent, shards, low, largest):
    factor_of = 1.0
    for axis_at, blocks in shards:
        heights = jax.random.uniform(jax.random.fold_in(jax.random.fold_in(rng, 6), axis_at), (blocks,), jnp.float32, low / len(shards), largest / len(shards))
        factor_of = factor_of * jnp.repeat(jnp.exp(heights), extent[axis_at] // blocks).reshape((-1,) + (1,) * (len(extent) - 1 - axis_at))
    return factor_of


def gaussian(own_key, shape, spread, bound, shards=(), held_as=jnp.bfloat16):
    drawn = jax.random.normal(own_key, shape, jnp.float32) * spread
    if len(shards) > 0:
        drawn = level_of(own_key, shape, shards, -0.22, 0.18) * drawn
    return jnp.clip(drawn, min=-bound, max=bound).astype(held_as)


def setup_inputs(seed: int = 0) -> dict:
    key_of = jax.random.split(jax.random.key(seed), 12)
    return {
        "layer_in": gaussian(key_of[0], (SEQLEN, D), 1.0, 6.0, ((0, 64), (1, 4))),
        "attn_gain": jnp.clip(1.0 + 0.18 * jax.random.normal(key_of[1], (D,), jnp.float32), 0.1, 1.9),
        "qkv_weight": gaussian(key_of[2], (3, D, HEADS * DK), D ** -0.5, 0.125, ((2, 4),)),
        "log_decay": draw_log_decay(jax.random.fold_in(key_of[11], 71), 0),
        "write_rate": draw_write_rate(jax.random.fold_in(key_of[11], 71), 0),
        "head_gain": jnp.clip(1.0 + 0.18 * jax.random.normal(key_of[5], (DK,), jnp.float32), 0.1, 1.9),
        "out_weight": gaussian(key_of[6], (HEADS * DK, D), (HEADS * DK) ** -0.5, 0.1875, ((0, 4),)),
        "ffn_gain": jnp.clip(1.0 + 0.18 * jax.random.normal(key_of[7], (D,), jnp.float32), 0.1, 1.9),
        "gate_weight": gaussian(key_of[8], (D, FF), D ** -0.5, 0.125, ((1, 4),)),
        "up_weight": gaussian(key_of[9], (D, FF), D ** -0.5, 0.125, ((1, 4),)),
        "down_weight": gaussian(key_of[10], (FF, D), FF ** -0.5, 0.125, ((0, 4),)),
    }


norm_floor = 0.1
head_floor = 0.05

def rms_scale(values, gain, floor):
    return values * lax.rsqrt(lax.optimization_barrier(jnp.mean(values * values, axis=-1, keepdims=True)) + floor) * gain

def unit_rows(vectors):
    return vectors * lax.rsqrt(lax.optimization_barrier(jnp.sum(vectors * vectors, axis=-1, keepdims=True)) + 1.0)

def grouped_sum(left_side, right_side, groups):
    group_span = right_side.shape[0] // groups
    running = jnp.zeros((left_side.shape[0], right_side.shape[1]), jnp.float32)
    for member in range(groups):
        partial_value = jnp.dot(left_side[:, member * group_span:(member + 1) * group_span], right_side[member * group_span:(member + 1) * group_span], preferred_element_type=jnp.float32)
        running = running + partial_value.astype(jnp.bfloat16).astype(jnp.float32)
    return running

def token_step(memory, inputs):
    queries, key_rows, values, decay_step, write_step = inputs
    projected = lax.optimization_barrier(jnp.sum(key_rows[:, :, None] * memory, axis=1))
    memory = decay_step[:, None, None] * (memory - write_step[:, None, None] * key_rows[:, :, None] * projected[:, None, :]) + write_step[:, None, None] * key_rows[:, :, None] * values[:, None, :]
    output = lax.optimization_barrier(jnp.sum(queries[:, :, None] * memory, axis=1))
    return (memory, output)

def reference(layer_in, attn_gain, qkv_weight, log_decay, write_rate, head_gain, out_weight, ffn_gain, gate_weight, up_weight, down_weight):
    inputs = layer_in.astype(jnp.float32)
    normed = rms_scale(inputs, attn_gain, norm_floor).astype(jnp.bfloat16)
    queries = jnp.dot(normed, qkv_weight[0], preferred_element_type=jnp.float32).reshape(SEQLEN, HEADS, DK)
    key_rows = jnp.dot(normed, qkv_weight[1], preferred_element_type=jnp.float32).reshape(SEQLEN, HEADS, DK)
    values = jnp.dot(normed, qkv_weight[2], preferred_element_type=jnp.float32).reshape(SEQLEN, HEADS, DK)
    queries = unit_rows(queries)
    key_rows = unit_rows(key_rows)
    start = jnp.zeros((HEADS, DK, DK), jnp.float32)
    final_memory, heads_raw = lax.scan(token_step, start, (queries, key_rows, values, jnp.exp(log_decay).T, write_rate.T))
    heads_out = rms_scale(heads_raw, head_gain, head_floor).reshape(SEQLEN, HEADS * DK).astype(jnp.bfloat16)
    attn = grouped_sum(heads_out, out_weight, N_TP)
    residual = inputs + attn
    normed_mid = rms_scale(residual, ffn_gain, norm_floor).astype(jnp.bfloat16)
    gate_act = jnp.dot(normed_mid, gate_weight, preferred_element_type=jnp.float32)
    up_act = jnp.dot(normed_mid, up_weight, preferred_element_type=jnp.float32)
    hidden = (jax.nn.silu(gate_act) * up_act).astype(jnp.bfloat16)
    ffn = grouped_sum(hidden, down_weight, N_TP)
    return (residual + ffn).astype(jnp.bfloat16)
```

```python
import functools

import jax
import jax.numpy as jnp
from jax import lax
from jax.experimental import pallas as pl
from jax.experimental.pallas import tpu as pltpu
from jax.sharding import Mesh
from jax.sharding import PartitionSpec as P

SEQ = ("seq_0", "seq_1", "seq_2")
MESH = pl.DeviceIdType.MESH
BF16 = jnp.bfloat16
F32 = jnp.float32

norm_floor = 0.1
head_floor = 0.05
SPAN = 128
BASE = 8


def mm(a, b, dims=((1,), (0,))):
    return lax.dot_general(
        a.astype(BF16), b.astype(BF16), (dims, ((), ())), preferred_element_type=F32
    )


def mm_exact(a, b):
    return lax.dot_general(
        a, b, (((1,), (0,)), ((), ())), preferred_element_type=F32, precision=lax.Precision.HIGHEST
    )


def mm_split(a, b):
    a_high, b_high = (a.astype(BF16), b.astype(BF16))
    a_low = (a - a_high.astype(F32)).astype(BF16)
    b_low = (b - b_high.astype(F32)).astype(BF16)
    return mm(a_high, b_high) + (mm(a_high, b_low) + mm(a_low, b_high))


def unit_rows(vectors):
    return vectors * lax.rsqrt(jnp.sum(vectors * vectors, axis=-1, keepdims=True) + 1.0)


def iotas(size):
    rows = lax.broadcasted_iota(jnp.int32, (size, size), 0)
    cols = lax.broadcasted_iota(jnp.int32, (size, size), 1)
    return (rows, cols)


def inverses(lowers):
    size = lowers[0].shape[0]
    rows, cols = iotas(size)
    same = rows // BASE == cols // BASE
    powers = [jnp.where(same, a, 0.0) for a in lowers]
    found = [jnp.where(rows == cols, 1.0, 0.0) - p for p in powers]
    reach = 2
    while reach < BASE:
        powers = [mm_split(p, p) for p in powers]
        found = [x + mm_split(x, p) for x, p in zip(found, powers)]
        reach *= 2
    block = BASE
    while block < size:
        pick = (rows // (2 * block) == cols // (2 * block)) & (rows // block != cols // block)
        inner = [mm(jnp.where(pick, a, 0.0), x) for a, x in zip(lowers, found)]
        found = [x - mm(x, y) for x, y in zip(found, inner)]
        block *= 2
    return found


def compose(earlier, later):
    first_growth, first = earlier
    second_growth, second = later
    width = first.shape[0]
    second_map = second[:, :width]
    both_growth = jnp.concatenate([second_growth, second_growth], axis=1)
    own = jnp.concatenate([first_growth * second_map, second[:, width:]], axis=1)
    return (first_growth * second_growth, both_growth * first + own - mm(second_map, first))


def apply_terms(terms, state):
    growth, both = terms
    width = both.shape[0]
    return growth * state - mm(both[:, :width], state) + both[:, width:]


def packed(terms):
    growth, both = terms
    high = growth.astype(BF16).astype(F32)
    middle = (growth - high).astype(BF16).astype(F32)
    low = growth - high - middle
    width = both.shape[0]
    row = lax.broadcasted_iota(jnp.int32, (16, width), 0)
    parts = jnp.where(row == 0, high, jnp.where(row == 1, middle, jnp.where(row == 2, low, 0.0)))
    return jnp.concatenate([both, jnp.concatenate([parts, parts], axis=1)], axis=0).astype(BF16)


def unpacked(message):
    whole = message.astype(F32)
    width = whole.shape[1] // 2
    growth = whole[width : width + 1, :width]
    growth = growth + whole[width + 1 : width + 2, :width] + whole[width + 2 : width + 3, :width]
    return (growth, whole[:width])


def choose(first, terms, others):
    return tuple(jnp.where(first, a, b) for a, b in zip(terms, others))


def ring_gather(axis, size, held, send_sem, recv_sem, between):
    here = lax.axis_index(axis)
    right, left = (lax.rem(here + 1, size), lax.rem(here + size - 1, size))

    def copy(way, step):
        owner = lax.rem(here + size - step, size) if way == 0 else lax.rem(here + step, size)
        return pltpu.make_async_remote_copy(
            src_ref=held.at[owner],
            dst_ref=held.at[owner],
            send_sem=send_sem.at[way, step],
            recv_sem=recv_sem.at[way, step],
            device_id={axis: right if way == 0 else left},
            device_id_type=MESH,
        )

    steps = (size // 2, (size - 1) // 2)
    copies = [[copy(way, step) for step in range(steps[way])] for way in (0, 1)]
    for way in (0, 1):
        if steps[way]:
            copies[way][0].start()
    for step in range(steps[0]):
        between(step)
        for way in (0, 1):
            if step < steps[way]:
                copies[way][step].wait_recv()
                if step + 1 < steps[way]:
                    copies[way][step + 1].start()
    for way in (0, 1):
        for one in copies[way]:
            one.wait_send()


def layer_kernel(
    sizes,
    x_ref,
    attn_gain_ref,
    decay_ref,
    rate_ref,
    head_gain_ref,
    ffn_gain_ref,
    qkv_hbm,
    out_hbm,
    gate_hbm,
    up_hbm,
    down_hbm,
    o_ref,
    qkv_w,
    out_w,
    gate_w,
    up_w,
    down_w,
    rows_all,
    heads_all,
    local_out,
    entry_map,
    running,
    growth_now,
    pair_mine,
    pair_other,
    z_held,
    x_held,
    picked,
    picked_growth,
    states,
    parts,
    passing,
    joined,
    landed,
    resid,
    kept,
    load_sem,
    x_send,
    x_recv,
    h_send,
    h_recv,
    r_send,
    r_recv,
    w_send,
    w_recv,
    pair_send,
    pair_recv,
    z_send,
    z_recv,
    s_send,
    s_recv,
):
    x_size, z_size, tp_size, blocks = sizes
    me = lax.axis_index("tp")
    core = lax.axis_index("seq_2")
    z_here = lax.axis_index("seq_1")
    x_here = lax.axis_index("seq_0")
    right, left = (lax.rem(me + 1, tp_size), lax.rem(me + tp_size - 1, tp_size))
    opposite = lax.rem(me + 2, tp_size)
    width = head_gain_ref.shape[1]
    heads = local_out.shape[0]
    slice_width = x_ref.shape[1]
    shard_rows = heads * width
    half = SPAN // 2
    near = {"tp": right}, {"tp": left}

    loads = [
        pltpu.make_async_copy(qkv_hbm, qkv_w, load_sem.at[0]),
        pltpu.make_async_copy(out_hbm, out_w.at[pl.ds(me * shard_rows, shard_rows)], load_sem.at[1]),
        pltpu.make_async_copy(gate_hbm, gate_w, load_sem.at[2]),
        pltpu.make_async_copy(up_hbm, up_w, load_sem.at[3]),
        pltpu.make_async_copy(down_hbm, down_w, load_sem.at[4]),
    ]
    for load in loads:
        load.start()

    barrier = pltpu.get_barrier_semaphore()
    friends = [{"tp": right}, {"tp": left}, {"seq_2": 1 - core}]
    for axis, here, size in (("seq_1", z_here, z_size), ("seq_0", x_here, x_size)):
        friends.append({axis: lax.rem(here + 1, size)})
        friends.append({axis: lax.rem(here + size - 1, size)})
    for friend in friends:
        pl.semaphore_signal(barrier, inc=1, device_id=friend, device_id_type=MESH)
    pl.semaphore_wait(barrier, len(friends))

    def span_of(block, start=0, size=SPAN):
        return pl.ds(pl.multiple_of(block * SPAN + start, half), size)

    def remote(source, target, send, recv, device):
        return pltpu.make_async_remote_copy(
            src_ref=source,
            dst_ref=target,
            send_sem=send,
            recv_sem=recv,
            device_id=device,
            device_id_type=MESH,
        )

    def x_first(block, way):
        there = rows_all.at[me, span_of(block)]
        return remote(
            x_ref.at[span_of(block)], there, x_send.at[way, block], x_recv.at[way, block], near[way]
        )

    def x_second(block, way):
        owner = left if way == 0 else right
        there = rows_all.at[owner, span_of(block, way * half, half)]
        return remote(
            there, there, x_send.at[2 + way, block], x_recv.at[2 + way, block], near[way]
        )

    def h_first(block, way):
        there = heads_all.at[me, span_of(block)]
        return remote(there, there, h_send.at[way, block], h_recv.at[way, block], near[way])

    def h_second(block, way):
        owner = left if way == 0 else right
        there = heads_all.at[owner, span_of(block, way * half, half)]
        return remote(
            there, there, h_send.at[2 + way, block], h_recv.at[2 + way, block], near[way]
        )

    def project(block):
        spread = [rows_all[j, span_of(block), :].astype(F32) for j in range(tp_size)]
        squares = sum(jnp.sum(part * part, axis=1, keepdims=True) for part in spread)
        scale = lax.rsqrt(squares * (1.0 / (tp_size * slice_width)) + norm_floor)
        normed = jnp.concatenate(
            [
                (part * scale * attn_gain_ref[:, j * slice_width : (j + 1) * slice_width]).astype(
                    BF16
                )
                for j, part in enumerate(spread)
            ],
            axis=1,
        )
        return [
            jnp.dot(normed, qkv_w[i], preferred_element_type=F32) for i in range(3)
        ]

    def recur(block):
        projected = project(block)
        rows, cols = iotas(SPAN)
        ones = jnp.ones((SPAN, SPAN), F32)
        upper = jnp.where(rows <= cols, 1.0, 0.0)
        cut = [[part[:, h * width : (h + 1) * width] for h in range(heads)] for part in projected]
        queries = [unit_rows(part) for part in cut[0]]
        keys = [unit_rows(part) for part in cut[1]]
        values = cut[2]
        decay = [decay_ref[h * blocks + block] for h in range(heads)]
        rate = [rate_ref[h * blocks + block] for h in range(heads)]
        along = [mm_exact(d, upper)[0:1] for d in decay]
        total = [mm_exact(d, ones)[0:1] for d in decay]
        down = [mm_exact(jnp.where(rows >= cols, d[0:1], 0.0), ones) for d in decay]
        beta = [mm_exact(jnp.where(rows == cols, r[0:1], 0.0), ones) for r in rate]
        fade = [
            jnp.where(rows >= cols, jnp.exp(jnp.minimum(d - a, 0.0)), 0.0)
            for d, a in zip(down, along)
        ]
        key_key = [mm(k, k, ((1,), (1,))) for k in keys]
        query_key = [mm(q, k, ((1,), (1,))) for q, k in zip(queries, keys)]
        lowers = [
            jnp.where(rows > cols, b * kk * f, 0.0) for b, kk, f in zip(beta, key_key, fade)
        ]
        inverse = inverses(lowers)
        grown = [jnp.exp(d) for d in down]
        sides = [
            jnp.concatenate([(b * g) * k, b * v], axis=1)
            for b, g, k, v in zip(beta, grown, keys, values)
        ]
        solved = [mm(x, s) for x, s in zip(inverse, sides)]
        tails = [k * jnp.exp(t - d) for k, t, d in zip(keys, total, down)]
        terms = [
            (jnp.exp(t), mm(k, s, ((0,), (0,)))) for t, k, s in zip(total, tails, solved)
        ]
        mixed = [mm(qk * f, s) for qk, f, s in zip(query_key, fade, solved)]
        for h in range(heads):
            entry = grown[h] * queries[h] - mixed[h][:, :width]
            growth = growth_now[h][0:1]
            before = running[h]
            reached = mm(entry, before)
            local_out[h, span_of(block), :] = mixed[h][:, width:] + reached[:, width:]
            entry_map[h, span_of(block), :] = (growth * entry - reached[:, :width]).astype(BF16)
            new_growth, new_terms = compose((growth, before), terms[h])
            running[h] = new_terms
            growth_now[h] = jnp.broadcast_to(new_growth, growth_now.shape[1:])

    rows_all[me] = x_ref[...]
    running[...] = jnp.zeros_like(running)
    growth_now[...] = jnp.ones_like(growth_now)
    for block in range(min(2, blocks)):
        for way in (0, 1):
            x_first(block, way).start()
    loads[0].wait()

    @pl.loop(0, blocks + 1)
    def _(block):
        @pl.when(block < blocks)
        def _():
            for way in (0, 1):
                x_first(block, way).wait_recv()
                x_second(block, way).start()

        @pl.when(block + 2 < blocks)
        def _():
            for way in (0, 1):
                x_first(block + 2, way).start()

        @pl.when(block > 0)
        def _():
            for way in (0, 1):
                x_second(block - 1, way).wait_recv()
            recur(block - 1)

    part_rows = shard_rows // 2

    def w_piece(owner, start, size):
        first = pl.multiple_of(owner * shard_rows + core * part_rows + start, part_rows // 2)
        return out_w.at[pl.ds(first, size)]

    def w_copy(index, piece, device):
        return remote(piece, piece, w_send.at[index], w_recv.at[index], device)

    partner = {"seq_2": 1 - core}
    w_first = [w_copy(way, w_piece(me, 0, part_rows), near[way]) for way in (0, 1)]
    w_second = [
        w_copy(2, w_piece(left, 0, part_rows // 2), near[0]),
        w_copy(3, w_piece(right, part_rows // 2, part_rows // 2), near[1]),
    ]
    w_across = [
        w_copy(4 + n, w_piece(owner, 0, part_rows), partner)
        for n, owner in enumerate((left, right, opposite))
    ]
    loads[1].wait()
    for one in w_first:
        one.start()

    for h in range(heads):
        pair_mine[h] = packed((growth_now[h][0:1], running[h]))
    pair_copy = remote(pair_mine, pair_other, pair_send.at[0], pair_recv.at[0], partner)
    pair_copy.start()
    pair_copy.wait_recv()
    own, other = (unpacked(pair_mine[core]), unpacked(pair_other[core]))
    z_held[z_here] = packed(compose(choose(core == 0, own, other), choose(core == 0, other, own)))

    def idle(step):
        pass

    ring_gather("seq_1", z_size, z_held, z_send, z_recv, idle)

    running_now = (jnp.ones((1, width), F32), jnp.zeros((width, 2 * width), F32))
    for j in range(z_size):

        @pl.when(z_here == j)
        def _(now=running_now):
            picked_growth[...] = jnp.broadcast_to(now[0], picked_growth.shape)
            picked[...] = now[1]

        running_now = compose(running_now, unpacked(z_held[j]))
    x_held[x_here] = packed(running_now)
    for one in w_first:
        one.wait_recv()
    for one in w_second:
        one.start()
    for one in w_across[:2]:
        one.start()
    ring_gather("seq_0", x_size, x_held, s_send, s_recv, idle)
    state = jnp.zeros((width, width), F32)
    chosen = state
    for j in range(x_size):
        chosen = jnp.where(x_here == j, state, chosen)
        if j + 1 < x_size:
            state = apply_terms(unpacked(x_held[j]), state)
    states[core] = apply_terms((picked_growth[0:1], picked[...]), chosen)
    state_copy = remote(
        states.at[core], states.at[core], pair_send.at[1], pair_recv.at[1], partner
    )
    state_copy.start()
    for one in w_second:
        one.wait_recv()
    w_across[2].start()
    state_in = remote(
        states.at[1 - core], states.at[1 - core], pair_send.at[1], pair_recv.at[1], partner
    )
    state_in.wait_recv()
    starts = [
        jnp.where(core == 0, states[h], apply_terms(unpacked(pair_other[h]), states[h])).astype(
            BF16
        )
        for h in range(heads)
    ]

    for block in range(blocks):
        outs = []
        for h in range(heads):
            raw = local_out[h, span_of(block), :] + mm(entry_map[h, span_of(block), :], starts[h])
            level = jnp.mean(raw * raw, axis=-1, keepdims=True)
            outs.append((raw * lax.rsqrt(level + head_floor) * head_gain_ref[...]).astype(BF16))
        heads_all[me, span_of(block), :] = jnp.concatenate(outs, axis=1)
        if block < 2:
            for way in (0, 1):
                h_first(block, way).start()

    for one in w_across:
        one.wait_recv()
    for load in loads[2:]:
        load.wait()

    def r_far(block, way):
        return remote(
            parts.at[block, opposite, pl.ds(way * half, half)],
            passing.at[way, block],
            r_send.at[way, block],
            r_recv.at[way, block],
            near[way],
        )

    def r_direct(block, way):
        target = right if way == 0 else left
        piece = pl.ds((1 - way) * half, half)
        return remote(
            parts.at[block, target, piece],
            landed.at[way, block, piece],
            r_send.at[2 + way, block],
            r_recv.at[2 + way, block],
            near[way],
        )

    def r_joined(block, way):
        return remote(
            joined.at[way, block],
            landed.at[way, block, pl.ds(way * half, half)],
            r_send.at[4 + way, block],
            r_recv.at[4 + way, block],
            near[way],
        )

    def feed_forward(block):
        attended = jnp.concatenate(
            [heads_all[j, span_of(block), :] for j in range(tp_size)], axis=1
        )
        squares = jnp.zeros((SPAN, 1), F32)
        for j in range(tp_size):
            piece = rows_all[j, span_of(block), :].astype(F32) + jnp.dot(
                attended,
                out_w[:, j * slice_width : (j + 1) * slice_width],
                preferred_element_type=F32,
            )
            resid[j] = piece
            squares = squares + jnp.sum(piece * piece, axis=1, keepdims=True)
        scale = lax.rsqrt(squares * (1.0 / (tp_size * slice_width)) + norm_floor)
        normed = jnp.concatenate(
            [
                (
                    resid[j] * scale * ffn_gain_ref[:, j * slice_width : (j + 1) * slice_width]
                ).astype(BF16)
                for j in range(tp_size)
            ],
            axis=1,
        )
        kept[span_of(block), :] = resid[me]
        gate_act = jnp.dot(normed, gate_w[...], preferred_element_type=F32)
        up_act = jnp.dot(normed, up_w[...], preferred_element_type=F32)
        hidden = (jax.nn.silu(gate_act) * up_act).astype(BF16)
        for j in range(tp_size):
            parts[block, j] = jnp.dot(
                hidden,
                down_w[:, j * slice_width : (j + 1) * slice_width],
                preferred_element_type=F32,
            ).astype(BF16)

    def join(block):
        for way in (0, 1):
            r_far(block, way).wait_recv()
            target = right if way == 0 else left
            joined[way, block] = (
                passing[way, block].astype(F32)
                + parts[block, target, pl.ds(way * half, half), :].astype(F32)
            ).astype(BF16)
            r_joined(block, way).start()

    def finish(block):
        for way in (0, 1):
            r_direct(block, way).wait_recv()
            r_joined(block, way).wait_recv()
        total = kept[span_of(block), :] + parts[block, me].astype(F32)
        total = total + landed[0, block].astype(F32) + landed[1, block].astype(F32)
        o_ref[span_of(block), :] = total.astype(BF16)

    @pl.loop(0, blocks + 3)
    def _(block):
        @pl.when(block < blocks)
        def _():
            for way in (0, 1):
                h_first(block, way).wait_recv()
                h_second(block, way).start()

        @pl.when(block + 2 < blocks)
        def _():
            for way in (0, 1):
                h_first(block + 2, way).start()

        @pl.when((block > 1) & (block < blocks + 2))
        def _():
            join(block - 2)

        @pl.when((block > 0) & (block < blocks + 1))
        def _():
            for way in (0, 1):
                h_second(block - 1, way).wait_recv()
            feed_forward(block - 1)
            for way in (0, 1):
                r_far(block - 1, way).start()
                r_direct(block - 1, way).start()

        @pl.when(block > 2)
        def _():
            finish(block - 3)

    @pl.loop(0, blocks)
    def _(block):
        for way in (0, 1):
            x_first(block, way).wait_send()
            x_second(block, way).wait_send()
            h_first(block, way).wait_send()
            h_second(block, way).wait_send()
            r_far(block, way).wait_send()
            r_direct(block, way).wait_send()
            r_joined(block, way).wait_send()

    for one in w_first + w_second + w_across + [pair_copy, state_copy]:
        one.wait_send()


def body(
    sizes,
    layer_in,
    attn_gain,
    qkv_weight,
    log_decay,
    write_rate,
    head_gain,
    out_weight,
    ffn_gain,
    gate_weight,
    up_weight,
    down_weight,
):
    x_size, z_size, tp_size = sizes
    length, slice_width = layer_in.shape
    full = tp_size * slice_width
    width = head_gain.shape[0]
    heads = qkv_weight.shape[2] // width
    blocks = length // SPAN
    hidden = gate_weight.shape[1]
    shard_rows = out_weight.shape[0]

    def rows_of(per_token):
        return jnp.broadcast_to(
            per_token.reshape(heads * blocks, 1, SPAN), (heads * blocks, 8, SPAN)
        )

    vmem = pl.BlockSpec(memory_space=pltpu.VMEM)
    anywhere = pl.BlockSpec(memory_space=pl.ANY)
    dma = pltpu.SemaphoreType.DMA
    scratch = [
        pltpu.VMEM(qkv_weight.shape, BF16),
        pltpu.VMEM((tp_size * shard_rows, full), BF16),
        pltpu.VMEM(gate_weight.shape, BF16),
        pltpu.VMEM(up_weight.shape, BF16),
        pltpu.VMEM(down_weight.shape, BF16),
        pltpu.VMEM((tp_size, length, slice_width), BF16),
        pltpu.VMEM((tp_size, length, heads * width), BF16),
        pltpu.VMEM((heads, length, width), F32),
        pltpu.VMEM((heads, length, width), BF16),
        pltpu.VMEM((heads, width, 2 * width), F32),
        pltpu.VMEM((heads, 8, width), F32),
        pltpu.VMEM((heads, width + 16, 2 * width), BF16),
        pltpu.VMEM((heads, width + 16, 2 * width), BF16),
        pltpu.VMEM((z_size, width + 16, 2 * width), BF16),
        pltpu.VMEM((x_size, width + 16, 2 * width), BF16),
        pltpu.VMEM((width, 2 * width), F32),
        pltpu.VMEM((8, width), F32),
        pltpu.VMEM((heads, width, width), F32),
        pltpu.VMEM((blocks, tp_size, SPAN, slice_width), BF16),
        pltpu.VMEM((2, blocks, SPAN // 2, slice_width), BF16),
        pltpu.VMEM((2, blocks, SPAN // 2, slice_width), BF16),
        pltpu.VMEM((2, blocks, SPAN, slice_width), BF16),
        pltpu.VMEM((tp_size, SPAN, slice_width), F32),
        pltpu.VMEM((length, slice_width), F32),
        dma((5,)),
        dma((4, blocks)),
        dma((4, blocks)),
        dma((4, blocks)),
        dma((4, blocks)),
        dma((6, blocks)),
        dma((6, blocks)),
        dma((7,)),
        dma((7,)),
        dma((2,)),
        dma((2,)),
        dma((2, z_size)),
        dma((2, z_size)),
        dma((2, x_size)),
        dma((2, x_size)),
    ]
    return pl.pallas_call(
        functools.partial(layer_kernel, (x_size, z_size, tp_size, blocks)),
        out_shape=jax.ShapeDtypeStruct((length, slice_width), BF16),
        in_specs=[vmem] * 6 + [anywhere] * 5,
        out_specs=vmem,
        scratch_shapes=scratch,
        compiler_params=pltpu.CompilerParams(
            collective_id=0, has_side_effects=True, vmem_limit_bytes=60 * 1024 * 1024
        ),
        name="layer",
    )(
        layer_in,
        attn_gain.reshape(1, full),
        rows_of(log_decay),
        rows_of(write_rate),
        head_gain.reshape(1, width),
        ffn_gain.reshape(1, full),
        qkv_weight,
        out_weight,
        gate_weight,
        up_weight,
        down_weight,
    )


def layer(shape, tp_size):
    x_size, z_size, cores = shape
    in_specs = (
        P(SEQ, "tp"),
        P(),
        P(None, None, "tp"),
        P("tp", SEQ),
        P("tp", SEQ),
        P(),
        P("tp", None),
        P(),
        P(None, "tp"),
        P(None, "tp"),
        P("tp", None),
    )
    return functools.partial(body, (x_size, z_size, tp_size)), in_specs, P(SEQ, "tp")


def solution(mesh):
    torus = Mesh(mesh.devices.reshape(4, 8, 2, mesh.shape["tp"]), (*SEQ, "tp"))
    function, in_specs, out_specs = layer((4, 8, 2), mesh.shape["tp"])
    return jax.shard_map(
        function, mesh=torus, in_specs=in_specs, out_specs=out_specs, check_vma=False
    )
```

```python
import functools

import jax
import jax.numpy as jnp
from jax import lax
from jax.experimental import pallas as pl
from jax.experimental.pallas import tpu as pltpu
from jax.sharding import Mesh
from jax.sharding import PartitionSpec as P

SEQ = ("seq_0", "seq_1", "seq_2")
MESH = pl.DeviceIdType.MESH
BF16 = jnp.bfloat16
F32 = jnp.float32

norm_floor = 0.1
head_floor = 0.05
SPAN = 128
GROUP = 2
AHEAD = 2


def mm(a, b, dims=((1,), (0,))):
    return lax.dot_general(
        a.astype(BF16), b.astype(BF16), (dims, ((), ())), preferred_element_type=F32
    )


def mm_exact(a, b):
    return lax.dot_general(
        a, b, (((1,), (0,)), ((), ())), preferred_element_type=F32, precision=lax.Precision.HIGHEST
    )


def unit_rows(vectors):
    return vectors * lax.rsqrt(jnp.sum(vectors * vectors, axis=-1, keepdims=True) + 1.0)


def iotas(size):
    rows = lax.broadcasted_iota(jnp.int32, (size, size), 0)
    cols = lax.broadcasted_iota(jnp.int32, (size, size), 1)
    return (rows, cols)


def inverses(lowers):
    size = lowers[0].shape[0]
    rows, cols = iotas(size)
    pairs = rows // 2 == cols // 2
    found = [jnp.where(rows == cols, 1.0, jnp.where(pairs, -a, 0.0)) for a in lowers]
    block = 2
    while block < size:
        pick = (rows // (2 * block) == cols // (2 * block)) & (rows // block != cols // block)
        inner = [mm(jnp.where(pick, a, 0.0), x) for a, x in zip(lowers, found)]
        found = [x - mm(x, y) for x, y in zip(found, inner)]
        block *= 2
    return found


def compose(earlier, later):
    first_growth, first = earlier
    second_growth, second = later
    width = first.shape[0]
    second_map = second[:, :width]
    both_growth = jnp.concatenate([second_growth, second_growth], axis=1)
    own = jnp.concatenate([first_growth * second_map, second[:, width:]], axis=1)
    return (first_growth * second_growth, both_growth * first + own - mm(second_map, first))


def apply_terms(terms, state):
    growth, both = terms
    width = both.shape[0]
    return growth * state - mm(both[:, :width], state) + both[:, width:]


def packed(terms):
    growth, both = terms
    high = growth.astype(BF16).astype(F32)
    middle = (growth - high).astype(BF16).astype(F32)
    low = growth - high - middle
    width = both.shape[0]
    row = lax.broadcasted_iota(jnp.int32, (16, width), 0)
    parts = jnp.where(row == 0, high, jnp.where(row == 1, middle, jnp.where(row == 2, low, 0.0)))
    return jnp.concatenate([both[:, :width], parts], axis=0).astype(BF16), both[:, width:].astype(BF16)


def keep(message, terms):
    upper, lower = packed(terms)
    message[0] = upper
    message[1, pl.ds(0, lower.shape[0]), :] = lower


def unpacked(message):
    width = message.shape[2]
    upper = message[0].astype(F32)
    growth = upper[width : width + 1] + upper[width + 1 : width + 2] + upper[width + 2 : width + 3]
    lower = message[1, pl.ds(0, width), :].astype(F32)
    return (growth, jnp.concatenate([upper[:width], lower], axis=1))


def choose(first, terms, others):
    return tuple(jnp.where(first, a, b) for a, b in zip(terms, others))


def ring_gather(axis, size, held, send_sem, recv_sem, arrived):
    here = lax.axis_index(axis)
    right, left = (lax.rem(here + 1, size), lax.rem(here + size - 1, size))
    width = held.shape[3]

    def copy(way, step, part):
        owner = lax.rem(here + size - step, size) if way == 0 else lax.rem(here + step, size)
        piece = held.at[owner, part, pl.ds(0, width + 16 if part == 0 else width)]
        return pltpu.make_async_remote_copy(
            src_ref=piece,
            dst_ref=piece,
            send_sem=send_sem.at[way, part, step],
            recv_sem=recv_sem.at[way, part, step],
            device_id={axis: right if way == 0 else left},
            device_id_type=MESH,
        )

    steps = size // 2
    order = ((0, 1), (1, 0))
    copies = [
        [
            {
                part: copy(way, step, part)
                for part in order[way]
                if part == way or 2 * (step + 1) < size
            }
            for step in range(steps)
        ]
        for way in (0, 1)
    ]
    for n in (0, 1):
        for way in (0, 1):
            if order[way][n] in copies[way][0]:
                copies[way][0][order[way][n]].start()
    arrived(-1, ())
    for step in range(steps):
        for n in (0, 1):
            for way in (0, 1):
                part = order[way][n]
                if part in copies[way][step]:
                    copies[way][step][part].wait_recv()
                    if step + 1 < steps and part in copies[way][step + 1]:
                        copies[way][step + 1][part].start()
        arrived(step, (0, 1) if 2 * (step + 1) < size else (0,))
    return [one for way in copies for step in way for one in step.values()]


def layer_kernel(
    sizes,
    x_ref,
    attn_gain_ref,
    decay_ref,
    rate_ref,
    head_gain_ref,
    ffn_gain_ref,
    qkv_hbm,
    out_hbm,
    gate_hbm,
    up_hbm,
    down_hbm,
    o_ref,
    qkv_w,
    out_w,
    gate_w,
    up_w,
    down_w,
    rows_all,
    terms_all,
    running,
    growth_now,
    fade_of,
    system_of,
    grown_of,
    side_of,
    rate_of,
    tail_of,
    total_of,
    pair_mine,
    pair_other,
    z_held,
    x_held,
    states,
    leaving,
    parts,
    passing,
    joined,
    landed,
    resid,
    kept,
    load_sem,
    x_send,
    x_recv,
    h_send,
    h_recv,
    r_send,
    r_recv,
    w_send,
    w_recv,
    wz_send,
    wz_recv,
    wx_send,
    wx_recv,
    st_send,
    st_recv,
    pair_send,
    pair_recv,
    z_send,
    z_recv,
    s_send,
    s_recv,
):
    x_size, z_size, tp_size, blocks = sizes
    me = lax.axis_index("tp")
    core = lax.axis_index("seq_2")
    z_here = lax.axis_index("seq_1")
    x_here = lax.axis_index("seq_0")
    right, left = (lax.rem(me + 1, tp_size), lax.rem(me + tp_size - 1, tp_size))
    opposite = lax.rem(me + 2, tp_size)
    width = head_gain_ref.shape[1]
    heads = decay_ref.shape[0]
    slice_width = x_ref.shape[1]
    shard_rows = heads * width
    half = SPAN // 2
    near = {"tp": right}, {"tp": left}

    loads = [
        pltpu.make_async_copy(qkv_hbm, qkv_w, load_sem.at[0]),
        pltpu.make_async_copy(out_hbm, out_w.at[0], load_sem.at[1]),
        pltpu.make_async_copy(gate_hbm, gate_w, load_sem.at[2]),
        pltpu.make_async_copy(up_hbm, up_w, load_sem.at[3]),
        pltpu.make_async_copy(down_hbm, down_w, load_sem.at[4]),
    ]
    for load in loads:
        load.start()

    barrier = pltpu.get_barrier_semaphore()
    around = (right, left, opposite)
    friends = [{"tp": other} for other in around] + [{"seq_2": 1 - core}]
    friends += [{"tp": other, "seq_2": 1 - core} for other in around]
    for axis, here, size in (("seq_1", z_here, z_size), ("seq_0", x_here, x_size)):
        friends.append({axis: lax.rem(here + 1, size)})
        friends.append({axis: lax.rem(here + size - 1, size)})
    for friend in friends:
        pl.semaphore_signal(barrier, inc=1, device_id=friend, device_id_type=MESH)
    pl.semaphore_wait(barrier, len(friends))

    def span_of(block, start=0, size=SPAN):
        return pl.ds(pl.multiple_of(block * SPAN + start, half), size)

    def remote(source, target, send, recv, device):
        return pltpu.make_async_remote_copy(
            src_ref=source,
            dst_ref=target,
            send_sem=send,
            recv_sem=recv,
            device_id=device,
            device_id_type=MESH,
        )

    group = GROUP * SPAN
    groups = blocks // GROUP

    def group_of(block, start=0, size=group):
        return pl.ds(pl.multiple_of(block * group + start, half), size)

    def x_first(block, way):
        there = rows_all.at[me, group_of(block)]
        return remote(
            x_ref.at[group_of(block)], there, x_send.at[way, block], x_recv.at[way, block], near[way]
        )

    def x_second(block, way):
        owner = left if way == 0 else right
        there = rows_all.at[owner, group_of(block, way * group // 2, group // 2)]
        return remote(
            there, there, x_send.at[2 + way, block], x_recv.at[2 + way, block], near[way]
        )

    def t_first(block, way):
        there = terms_all.at[me, group_of(block)]
        return remote(there, there, h_send.at[way, block], h_recv.at[way, block], near[way])

    def t_second(block, way):
        owner = left if way == 0 else right
        there = terms_all.at[owner, group_of(block, way * group // 2, group // 2)]
        return remote(
            there, there, h_send.at[2 + way, block], h_recv.at[2 + way, block], near[way]
        )

    full = tp_size * slice_width
    core_rows = shard_rows // 2
    piece_rows = core_rows // z_size
    piece_cols = full // x_size

    def w_piece(z_at, x_at, start=0, size=piece_cols):
        first = pl.multiple_of(core * core_rows + z_at * piece_rows, piece_rows)
        return (
            pl.ds(first, piece_rows),
            pl.ds(pl.multiple_of(x_at * piece_cols + start, piece_cols // 2), size),
        )

    def w_column(x_at, start=0, size=piece_cols):
        return (
            pl.ds(pl.multiple_of(core * core_rows, core_rows), core_rows),
            pl.ds(pl.multiple_of(x_at * piece_cols + start, piece_cols // 2), size),
        )

    own_rows, own_cols = w_piece(z_here, x_here)
    w_cross = [
        remote(
            out_hbm.at[own_rows, own_cols],
            out_w.at[slot, own_rows, own_cols],
            w_send.at[n],
            w_recv.at[n],
            {"tp": other},
        )
        for n, (other, slot) in enumerate(zip(around, (2, 1, 3)))
    ]

    def w_ring(axis, here, size, region, send, recv):
        copies = []
        for step in range(size // 2):
            pair = []
            for way in (0, 1):
                owner = lax.rem(here + (size - step if way == 0 else step), size)
                last = 2 * (step + 1) == size
                half_cols = piece_cols // 2
                rows, cols = region(owner, way * half_cols, half_cols) if last else region(owner)
                there = out_w.at[pl.ds(1, tp_size - 1), rows, cols]
                onward = {axis: lax.rem(here + (1 if way == 0 else size - 1), size)}
                pair.append(remote(there, there, send.at[way, step], recv.at[way, step], onward))
            copies.append(pair)
        return copies

    w_z = w_ring(
        "seq_1", z_here, z_size, lambda at, *cut: w_piece(at, x_here, *cut), wz_send, wz_recv
    )
    w_x = w_ring("seq_0", x_here, x_size, w_column, wx_send, wx_recv)
    w_waves = [w_cross] + w_z + w_x
    half_out_w = out_w.at[pl.ds(1, tp_size - 1), pl.ds(pl.multiple_of(core * core_rows, core_rows), core_rows)]
    w_across = remote(half_out_w, half_out_w, w_send.at[3], w_recv.at[3], {"seq_2": 1 - core})

    def w_move(wave):
        for one in w_waves[wave]:
            one.wait_recv()
        for one in w_waves[wave + 1] if wave + 1 < len(w_waves) else [w_across]:
            one.start()

    def prepare(block):
        rows, cols = iotas(SPAN)
        ones = jnp.ones((SPAN, SPAN), F32)
        upper = jnp.where(rows <= cols, 1.0, 0.0)
        for h in range(heads):
            tokens = span_of(block)
            decay = jnp.broadcast_to(decay_ref[h : h + 1, tokens], (SPAN, SPAN))
            rate = jnp.broadcast_to(rate_ref[h : h + 1, tokens], (SPAN, SPAN))
            along = mm_exact(decay[0:8], upper)[0:1]
            total = mm_exact(decay[0:8], ones)[0:1]
            down = mm_exact(jnp.where(rows >= cols, decay, 0.0), ones)
            beta = mm_exact(jnp.where(rows == cols, rate, 0.0), ones)
            fade = jnp.where(rows >= cols, jnp.exp(jnp.minimum(down - along, 0.0)), 0.0)
            grown = jnp.exp(down)
            fade_of[h, tokens, :] = fade
            system_of[h, tokens, :] = jnp.where(rows > cols, beta * fade, 0.0)
            grown_of[h, tokens, :] = grown
            side_of[h, tokens, :] = beta * grown
            rate_of[h, tokens, :] = beta
            tail_of[h, tokens, :] = jnp.exp(total - down)
            total_of[h, block] = jnp.broadcast_to(jnp.exp(total), total_of.shape[2:])

    def project(block):
        tokens = group_of(block)
        spread = [rows_all[j, tokens, :].astype(F32) for j in range(tp_size)]
        squares = sum(jnp.sum(part * part, axis=1, keepdims=True) for part in spread)
        scale = lax.rsqrt(squares * (1.0 / (tp_size * slice_width)) + norm_floor)
        normed = jnp.concatenate(
            [
                (part * scale * attn_gain_ref[:, j * slice_width : (j + 1) * slice_width]).astype(
                    BF16
                )
                for j, part in enumerate(spread)
            ],
            axis=1,
        )
        return normed

    chains = [(c, h) for c in range(GROUP) for h in range(heads)]

    def cut(part):
        return [part[c * SPAN : (c + 1) * SPAN, h * width : (h + 1) * width] for c, h in chains]

    def recur(block):
        normed = project(block)
        spans = [span_of(block * GROUP + c) for c, h in chains]

        def stored(ref):
            return [ref[h, tokens, :] for (c, h), tokens in zip(chains, spans)]

        keys = [unit_rows(part) for part in cut(jnp.dot(normed, qkv_w[1], preferred_element_type=F32))]
        key_key = [mm(k, k, ((1,), (1,))) for k in keys]
        values = cut(jnp.dot(normed, qkv_w[2], preferred_element_type=F32))
        inverse = inverses([kk * f for kk, f in zip(key_key, stored(system_of))])
        sides = [
            jnp.concatenate([g * k, b * v], axis=1)
            for b, g, k, v in zip(stored(rate_of), stored(side_of), keys, values)
        ]
        solved = [mm(x, s).astype(BF16) for x, s in zip(inverse, sides)]
        tails = [k * t for k, t in zip(keys, stored(tail_of))]
        terms = [mm(k, s, ((0,), (0,))) for k, s in zip(tails, solved)]
        before = []
        for n, (c, h) in enumerate(chains):
            growth = growth_now[h][0:1]
            entry_terms = running[h]
            before.append((growth, entry_terms))
            step = total_of[h, block * GROUP + c][0:1]
            new_growth, new_terms = compose((growth, entry_terms), (step, terms[n]))
            running[h] = new_terms
            growth_now[h] = jnp.broadcast_to(new_growth, growth_now.shape[1:])
        return (block, spans, stored, normed, keys, solved, before)

    def query(known):
        block, spans, stored, normed, keys, solved, before = known
        queries = [unit_rows(part) for part in cut(jnp.dot(normed, qkv_w[0], preferred_element_type=F32))]
        query_key = [mm(q, k, ((1,), (1,))) for q, k in zip(queries, keys)]
        mixed = [mm(qk * f, s) for qk, f, s in zip(query_key, stored(fade_of), solved)]
        entries = [
            g * q - m[:, :width] for g, q, m in zip(stored(grown_of), queries, mixed)
        ]
        reached = [mm(e, b[1]) for e, b in zip(entries, before)]
        for n, ((c, h), tokens) in enumerate(zip(chains, spans)):
            local = mixed[n][:, width:] + reached[n][:, width:]
            onward = before[n][0] * entries[n] - reached[n][:, :width]
            terms_all[me, tokens, h * width : (h + 1) * width] = local.astype(BF16)
            terms_all[me, tokens, (heads + h) * width : (heads + h + 1) * width] = onward.astype(
                BF16
            )

    rows_all[me] = x_ref[...]
    running[...] = jnp.zeros_like(running)
    growth_now[...] = jnp.ones_like(growth_now)
    for one in w_cross:
        one.start()
    for block in range(min(AHEAD, groups)):
        for way in (0, 1):
            x_first(block, way).start()

    @pl.loop(0, blocks)
    def _(block):
        prepare(block)

    loads[0].wait()
    w_move(0)

    slots = [(n, when) for n in range(groups) for when in (("early", "late") if n else ("early",))]
    plan = list(zip(range(1, len(w_waves) - 2), slots))
    early = [(wave, n) for wave, (n, when) in plan if when == "early"]
    late = [(wave, n) for wave, (n, when) in plan if when == "late"]

    @pl.loop(0, groups)
    def _(block):
        for way in (0, 1):
            x_first(block, way).wait_recv()
            x_second(block, way).start()

        @pl.when(block + AHEAD < groups)
        def _():
            for way in (0, 1):
                x_first(block + AHEAD, way).start()

        for wave, at in early:

            @pl.when(block == at)
            def _(wave=wave):
                w_move(wave)

        @pl.when(block > 0)
        def _():
            for way in (0, 1):
                x_second(block - 1, way).wait_recv()
            query(recur(block - 1))

        for wave, at in late:

            @pl.when(block == at)
            def _(wave=wave):
                w_move(wave)

    for block in range(groups - 1):
        for way in (0, 1):
            t_first(block, way).start()
    for way in (0, 1):
        x_second(groups - 1, way).wait_recv()
    last = recur(groups - 1)
    w_left = len(w_waves) - 1 - len(early) - len(late)
    for wave in range(len(w_waves) - w_left, len(w_waves) - 1):
        w_move(wave)

    partner = {"seq_2": 1 - core}
    for h in range(heads):
        keep(pair_mine.at[h], (growth_now[h][0:1], running[h]))
    pair_copy = remote(pair_mine, pair_other, pair_send.at[0], pair_recv.at[0], partner)
    pair_copy.start()
    pair_copy.wait_recv()
    own, other = (unpacked(pair_mine.at[core]), unpacked(pair_other.at[core]))
    chip = compose(choose(core == 0, own, other), choose(core == 0, other, own))
    keep(z_held.at[z_here], chip)
    nothing = (jnp.ones((1, width), F32), jnp.zeros((width, 2 * width), F32))
    sums = {"before": [nothing, nothing], "after": [nothing, nothing]}

    def t_pass(block):
        for way in (0, 1):
            t_first(block, way).wait_recv()
            t_second(block, way).start()

    def z_arrived(step, ways):
        if step < 0:
            query(last)
            for way in (0, 1):
                t_first(groups - 1, way).start()
        if 0 < step < groups:
            t_pass(step - 1)
        for way in ways:
            earlier = z_here > step if way == 0 else z_here + 1 + step >= z_size
            owner = lax.rem(z_here + (z_size - 1 - step if way == 0 else 1 + step), z_size)
            item = unpacked(z_held.at[owner])
            so_far = choose(earlier, sums["before"][way], sums["after"][way])
            joint = compose(item, so_far) if way == 0 else compose(so_far, item)
            sums["before"][way] = choose(earlier, joint, sums["before"][way])
            sums["after"][way] = choose(earlier, sums["after"][way], joint)

    ring_copies = ring_gather("seq_1", z_size, z_held, z_send, z_recv, z_arrived)
    through = compose(sums["before"][1], sums["before"][0])
    rest = compose(sums["after"][1], sums["after"][0])
    keep(x_held.at[x_here], compose(compose(through, chip), rest))

    def x_arrived(step, ways):
        if step < 0:
            w_move(len(w_waves) - 1)
            for block in range(max(0, min(groups, z_size // 2) - 1), groups - 1):
                t_pass(block)
        if step == 0:
            t_pass(groups - 1)

    ring_copies += ring_gather("seq_0", x_size, x_held, s_send, s_recv, x_arrived)
    chosen = jnp.zeros((width, width), F32)
    for back in range(x_size - 1, 0, -1):
        owner = lax.rem(x_here + x_size - back, x_size)
        chosen = jnp.where(x_here >= back, apply_terms(unpacked(x_held.at[owner]), chosen), chosen)
    first_terms = choose(core == 0, own, other)
    reached = apply_terms(through, chosen)
    leaving[0] = reached.astype(BF16)
    leaving[1] = apply_terms(first_terms, reached).astype(BF16)
    states[me, core] = leaving[core]
    state_copies = []
    for n, device in enumerate(friends[:7]):
        there = core if n < 3 else 1 - core
        state_copies.append(
            remote(leaving.at[there], states.at[me, core], st_send.at[n], st_recv.at[n], device)
        )
    for n in (2, 6, 0, 1, 3, 4, 5):
        state_copies[n].start()
    for load in loads[1:]:
        load.wait()
    w_across.wait_recv()
    for block in range(groups):
        for way in (0, 1):
            t_second(block, way).wait_recv()
    for n, (origin, head) in enumerate(
        [(left, core), (right, core), (opposite, core)]
        + [(me, 1 - core)]
        + [(left, 1 - core), (right, 1 - core), (opposite, 1 - core)]
    ):
        remote(
            leaving.at[0], states.at[origin, head], st_send.at[n], st_recv.at[n], {"tp": right}
        ).wait_recv()

    def r_far(block, way):
        return remote(
            parts.at[block, opposite, pl.ds(way * half, half)],
            passing.at[way, block],
            r_send.at[way, block],
            r_recv.at[way, block],
            near[way],
        )

    def r_direct(block, way):
        target = right if way == 0 else left
        piece = pl.ds((1 - way) * half, half)
        return remote(
            parts.at[block, target, piece],
            landed.at[way, block, piece],
            r_send.at[2 + way, block],
            r_recv.at[2 + way, block],
            near[way],
        )

    def r_joined(block, way):
        return remote(
            joined.at[way, block],
            landed.at[way, block, pl.ds(way * half, half)],
            r_send.at[4 + way, block],
            r_recv.at[4 + way, block],
            near[way],
        )

    def feed_forward(block):
        outs = []
        for origin in (me, *around):
            for h in range(heads):
                local = terms_all[origin, span_of(block), h * width : (h + 1) * width]
                onward = terms_all[
                    origin, span_of(block), (heads + h) * width : (heads + h + 1) * width
                ]
                raw = local.astype(F32) + mm(onward, states[origin, h])
                level = jnp.mean(raw * raw, axis=-1, keepdims=True)
                outs.append((raw * lax.rsqrt(level + head_floor) * head_gain_ref[...]).astype(BF16))
        attended = jnp.concatenate(outs, axis=1)
        squares = jnp.zeros((SPAN, 1), F32)
        for j in range(tp_size):
            piece = rows_all[j, span_of(block), :].astype(F32) + jnp.dot(
                attended,
                out_w[:, :, j * slice_width : (j + 1) * slice_width].reshape(
                    tp_size * shard_rows, slice_width
                ),
                preferred_element_type=F32,
            )
            resid[j] = piece
            squares = squares + jnp.sum(piece * piece, axis=1, keepdims=True)
        scale = lax.rsqrt(squares * (1.0 / (tp_size * slice_width)) + norm_floor)
        normed = jnp.concatenate(
            [
                (
                    resid[j] * scale * ffn_gain_ref[:, j * slice_width : (j + 1) * slice_width]
                ).astype(BF16)
                for j in range(tp_size)
            ],
            axis=1,
        )
        kept[span_of(block), :] = resid[me]
        gate_act = jnp.dot(normed, gate_w[...], preferred_element_type=F32)
        up_act = jnp.dot(normed, up_w[...], preferred_element_type=F32)
        hidden = (jax.nn.silu(gate_act) * up_act).astype(BF16)
        for j in range(tp_size):
            parts[block, j] = jnp.dot(
                hidden,
                down_w[:, j * slice_width : (j + 1) * slice_width],
                preferred_element_type=F32,
            ).astype(BF16)

    def join(block):
        for way in (0, 1):
            r_far(block, way).wait_recv()
            target = right if way == 0 else left
            joined[way, block] = (
                passing[way, block].astype(F32)
                + parts[block, target, pl.ds(way * half, half), :].astype(F32)
            ).astype(BF16)
            r_joined(block, way).start()

    def finish(block):
        for way in (0, 1):
            r_direct(block, way).wait_recv()
            r_joined(block, way).wait_recv()
        total = kept[span_of(block), :] + parts[block, me].astype(F32)
        total = total + landed[0, block].astype(F32) + landed[1, block].astype(F32)
        o_ref[span_of(block), :] = total.astype(BF16)

    @pl.loop(0, blocks + 2)
    def _(block):
        @pl.when((block > 0) & (block < blocks + 1))
        def _():
            join(block - 1)

        @pl.when(block < blocks)
        def _():
            feed_forward(block)
            for way in (0, 1):
                r_far(block, way).start()
                r_direct(block, way).start()

        @pl.when(block > 1)
        def _():
            finish(block - 2)

    @pl.loop(0, blocks)
    def _(block):
        for way in (0, 1):
            r_far(block, way).wait_send()
            r_direct(block, way).wait_send()
            r_joined(block, way).wait_send()

    @pl.loop(0, groups)
    def _(block):
        for way in (0, 1):
            x_first(block, way).wait_send()
            x_second(block, way).wait_send()
            t_first(block, way).wait_send()
            t_second(block, way).wait_send()

    w_copies = [one for wave in w_waves for one in wave] + [w_across]
    for one in w_copies + state_copies + [pair_copy] + ring_copies:
        one.wait_send()


def body(
    sizes,
    layer_in,
    attn_gain,
    qkv_weight,
    log_decay,
    write_rate,
    head_gain,
    out_weight,
    ffn_gain,
    gate_weight,
    up_weight,
    down_weight,
):
    x_size, z_size, tp_size = sizes
    length, slice_width = layer_in.shape
    full = tp_size * slice_width
    width = head_gain.shape[0]
    heads = qkv_weight.shape[2] // width
    blocks = length // SPAN
    hidden = gate_weight.shape[1]
    shard_rows = out_weight.shape[0]

    vmem = pl.BlockSpec(memory_space=pltpu.VMEM)
    anywhere = pl.BlockSpec(memory_space=pl.ANY)
    dma = pltpu.SemaphoreType.DMA
    scratch = [
        pltpu.VMEM(qkv_weight.shape, BF16),
        pltpu.VMEM((tp_size, shard_rows, full), BF16),
        pltpu.VMEM(gate_weight.shape, BF16),
        pltpu.VMEM(up_weight.shape, BF16),
        pltpu.VMEM(down_weight.shape, BF16),
        pltpu.VMEM((tp_size, length, slice_width), BF16),
        pltpu.VMEM((tp_size, length, 2 * heads * width), BF16),
        pltpu.VMEM((heads, width, 2 * width), F32),
        pltpu.VMEM((heads, 8, width), F32),
        *[pltpu.VMEM((heads, length, SPAN), F32) for _ in range(6)],
        pltpu.VMEM((heads, blocks, 8, width), F32),
        pltpu.VMEM((heads, 2, width + 16, width), BF16),
        pltpu.VMEM((heads, 2, width + 16, width), BF16),
        pltpu.VMEM((z_size, 2, width + 16, width), BF16),
        pltpu.VMEM((x_size, 2, width + 16, width), BF16),
        pltpu.VMEM((tp_size, heads, width, width), BF16),
        pltpu.VMEM((2, width, width), BF16),
        pltpu.VMEM((blocks, tp_size, SPAN, slice_width), BF16),
        pltpu.VMEM((2, blocks, SPAN // 2, slice_width), BF16),
        pltpu.VMEM((2, blocks, SPAN // 2, slice_width), BF16),
        pltpu.VMEM((2, blocks, SPAN, slice_width), BF16),
        pltpu.VMEM((tp_size, SPAN, slice_width), F32),
        pltpu.VMEM((length, slice_width), F32),
        dma((5,)),
        dma((4, blocks // GROUP)),
        dma((4, blocks // GROUP)),
        dma((4, blocks // GROUP)),
        dma((4, blocks // GROUP)),
        dma((6, blocks)),
        dma((6, blocks)),
        dma((4,)),
        dma((4,)),
        dma((2, z_size // 2)),
        dma((2, z_size // 2)),
        dma((2, x_size // 2)),
        dma((2, x_size // 2)),
        dma((7,)),
        dma((7,)),
        dma((2,)),
        dma((2,)),
        dma((2, 2, z_size)),
        dma((2, 2, z_size)),
        dma((2, 2, x_size)),
        dma((2, 2, x_size)),
    ]
    return pl.pallas_call(
        functools.partial(layer_kernel, (x_size, z_size, tp_size, blocks)),
        out_shape=jax.ShapeDtypeStruct((length, slice_width), BF16),
        in_specs=[vmem] * 6 + [anywhere] * 5,
        out_specs=vmem,
        scratch_shapes=scratch,
        compiler_params=pltpu.CompilerParams(
            collective_id=0, has_side_effects=True, vmem_limit_bytes=60 * 1024 * 1024
        ),
        name="layer",
    )(
        layer_in,
        attn_gain.reshape(1, full),
        log_decay,
        write_rate,
        head_gain.reshape(1, width),
        ffn_gain.reshape(1, full),
        qkv_weight,
        out_weight,
        gate_weight,
        up_weight,
        down_weight,
    )


def layer(shape, tp_size):
    x_size, z_size, cores = shape
    in_specs = (
        P(SEQ, "tp"),
        P(),
        P(None, None, "tp"),
        P("tp", SEQ),
        P("tp", SEQ),
        P(),
        P("tp", None),
        P(),
        P(None, "tp"),
        P(None, "tp"),
        P("tp", None),
    )
    return functools.partial(body, (x_size, z_size, tp_size)), in_specs, P(SEQ, "tp")


def solution(mesh):
    torus = Mesh(mesh.devices.reshape(4, 8, 2, mesh.shape["tp"]), (*SEQ, "tp"))
    function, in_specs, out_specs = layer((4, 8, 2), mesh.shape["tp"])
    return jax.shard_map(
        function, mesh=torus, in_specs=in_specs, out_specs=out_specs, check_vma=False
    )
```

```python
import functools

import jax
import jax.numpy as jnp
from jax import lax
from jax.experimental import pallas as pl
from jax.experimental.pallas import tpu as pltpu
from jax.sharding import Mesh
from jax.sharding import PartitionSpec as P

SEQ = ("seq_0", "seq_1", "seq_2")
MESH = pl.DeviceIdType.MESH
BF16 = jnp.bfloat16
F32 = jnp.float32

norm_floor = 0.1
head_floor = 0.05
SPAN = 128
GROUP = 2
AHEAD = 3


def mm(a, b, dims=((1,), (0,))):
    return lax.dot_general(
        a.astype(BF16), b.astype(BF16), (dims, ((), ())), preferred_element_type=F32
    )


def mm_exact(a, b):
    return lax.dot_general(
        a, b, (((1,), (0,)), ((), ())), preferred_element_type=F32, precision=lax.Precision.HIGHEST
    )


def unit_rows(vectors):
    return vectors * lax.rsqrt(jnp.sum(vectors * vectors, axis=-1, keepdims=True) + 1.0)


def iotas(size):
    rows = lax.broadcasted_iota(jnp.int32, (size, size), 0)
    cols = lax.broadcasted_iota(jnp.int32, (size, size), 1)
    return (rows, cols)


def inverses(lowers):
    size = lowers[0].shape[0]
    rows, cols = iotas(size)
    pairs = rows // 2 == cols // 2
    found = [jnp.where(rows == cols, 1.0, jnp.where(pairs, -a, 0.0)) for a in lowers]
    block = 2
    while block < size:
        wide = min(4 * block, size)
        pick = (rows // wide == cols // wide) & (rows // block != cols // block)
        inner = [mm(x, jnp.where(pick, a, 0.0)) for a, x in zip(lowers, found)]
        near = [x - mm(n, x) for n, x in zip(inner, found)]
        twice = [mm(n, n) for n in inner]
        found = [x + mm(n, x) for n, x in zip(twice, near)]
        block *= 4
    return found


def compose(earlier, later):
    first_growth, first = earlier
    second_growth, second = later
    width = first.shape[0]
    second_map = second[:, :width]
    both_growth = jnp.concatenate([second_growth, second_growth], axis=1)
    own = jnp.concatenate([first_growth * second_map, second[:, width:]], axis=1)
    return (first_growth * second_growth, both_growth * first + own - mm(second_map, first))


def apply_terms(terms, state):
    growth, both = terms
    width = both.shape[0]
    return growth * state - mm(both[:, :width], state) + both[:, width:]


def packed(terms):
    growth, both = terms
    high = growth.astype(BF16).astype(F32)
    middle = (growth - high).astype(BF16).astype(F32)
    low = growth - high - middle
    width = both.shape[0]
    row = lax.broadcasted_iota(jnp.int32, (16, width), 0)
    parts = jnp.where(row == 0, high, jnp.where(row == 1, middle, jnp.where(row == 2, low, 0.0)))
    return jnp.concatenate([both[:, :width], parts], axis=0).astype(BF16), both[:, width:].astype(BF16)


def keep(message, terms):
    upper, lower = packed(terms)
    message[0] = upper
    message[1, pl.ds(0, lower.shape[0]), :] = lower


def unpacked(message):
    width = message.shape[2]
    upper = message[0].astype(F32)
    growth = upper[width : width + 1] + upper[width + 1 : width + 2] + upper[width + 2 : width + 3]
    lower = message[1, pl.ds(0, width), :].astype(F32)
    return (growth, jnp.concatenate([upper[:width], lower], axis=1))


def choose(first, terms, others):
    return tuple(jnp.where(first, a, b) for a, b in zip(terms, others))


def ring_gather(axis, size, held, send_sem, recv_sem, arrived):
    here = lax.axis_index(axis)
    right, left = (lax.rem(here + 1, size), lax.rem(here + size - 1, size))
    width = held.shape[3]

    def copy(way, step, part):
        owner = lax.rem(here + size - step, size) if way == 0 else lax.rem(here + step, size)
        piece = held.at[owner, part, pl.ds(0, width + 16 if part == 0 else width)]
        return pltpu.make_async_remote_copy(
            src_ref=piece,
            dst_ref=piece,
            send_sem=send_sem.at[way, part, step],
            recv_sem=recv_sem.at[way, part, step],
            device_id={axis: right if way == 0 else left},
            device_id_type=MESH,
        )

    steps = size // 2
    order = ((0, 1), (1, 0))
    copies = [
        [
            {
                part: copy(way, step, part)
                for part in order[way]
                if part == way or 2 * (step + 1) < size
            }
            for step in range(steps)
        ]
        for way in (0, 1)
    ]
    for n in (0, 1):
        for way in (0, 1):
            if order[way][n] in copies[way][0]:
                copies[way][0][order[way][n]].start()
    arrived(-1, ())
    for step in range(steps):
        for n in (0, 1):
            for way in (0, 1):
                part = order[way][n]
                if part in copies[way][step]:
                    copies[way][step][part].wait_recv()
                    if step + 1 < steps and part in copies[way][step + 1]:
                        copies[way][step + 1][part].start()
        arrived(step, (0, 1) if 2 * (step + 1) < size else (0,))
    return [one for way in copies for step in way for one in step.values()]


def layer_kernel(
    sizes,
    x_ref,
    attn_gain_ref,
    decay_ref,
    rate_ref,
    head_gain_ref,
    ffn_gain_ref,
    qkv_hbm,
    out_hbm,
    gate_hbm,
    up_hbm,
    down_hbm,
    o_ref,
    qkv_w,
    out_w,
    gate_w,
    up_w,
    down_w,
    rows_all,
    terms_all,
    running,
    growth_now,
    fade_of,
    system_of,
    grown_of,
    side_of,
    rate_of,
    tail_of,
    total_of,
    pair_mine,
    pair_other,
    z_held,
    x_held,
    states,
    leaving,
    parts,
    passing,
    joined,
    landed,
    resid,
    kept,
    load_sem,
    x_send,
    x_recv,
    h_send,
    h_recv,
    r_send,
    r_recv,
    w_send,
    w_recv,
    wz_send,
    wz_recv,
    wx_send,
    wx_recv,
    st_send,
    st_recv,
    pair_send,
    pair_recv,
    z_send,
    z_recv,
    s_send,
    s_recv,
):
    x_size, z_size, tp_size, blocks = sizes
    me = lax.axis_index("tp")
    core = lax.axis_index("seq_2")
    z_here = lax.axis_index("seq_1")
    x_here = lax.axis_index("seq_0")
    right, left = (lax.rem(me + 1, tp_size), lax.rem(me + tp_size - 1, tp_size))
    opposite = lax.rem(me + 2, tp_size)
    width = head_gain_ref.shape[1]
    heads = decay_ref.shape[0]
    slice_width = x_ref.shape[1]
    shard_rows = heads * width
    half = SPAN // 2
    near = {"tp": right}, {"tp": left}

    loads = [
        pltpu.make_async_copy(qkv_hbm, qkv_w, load_sem.at[0]),
        pltpu.make_async_copy(out_hbm, out_w.at[0], load_sem.at[1]),
        pltpu.make_async_copy(gate_hbm, gate_w, load_sem.at[2]),
        pltpu.make_async_copy(up_hbm, up_w, load_sem.at[3]),
        pltpu.make_async_copy(down_hbm, down_w, load_sem.at[4]),
    ]
    barrier = pltpu.get_barrier_semaphore()
    around = (right, left, opposite)
    friends = [{"tp": other} for other in around] + [{"seq_2": 1 - core}]
    friends += [{"tp": other, "seq_2": 1 - core} for other in around]
    for axis, here, size in (("seq_1", z_here, z_size), ("seq_0", x_here, x_size)):
        friends.append({axis: lax.rem(here + 1, size)})
        friends.append({axis: lax.rem(here + size - 1, size)})
    for friend in friends:
        pl.semaphore_signal(barrier, inc=1, device_id=friend, device_id_type=MESH)
    for load in loads:
        load.start()
    pl.semaphore_wait(barrier, len(friends))

    def span_of(block, start=0, size=SPAN):
        return pl.ds(pl.multiple_of(block * SPAN + start, half), size)

    def remote(source, target, send, recv, device):
        return pltpu.make_async_remote_copy(
            src_ref=source,
            dst_ref=target,
            send_sem=send,
            recv_sem=recv,
            device_id=device,
            device_id_type=MESH,
        )

    group = GROUP * SPAN
    groups = blocks // GROUP

    def group_of(block, start=0, size=group):
        return pl.ds(pl.multiple_of(block * group + start, half), size)

    def x_first(block, way):
        there = rows_all.at[me, span_of(block)]
        return remote(
            x_ref.at[span_of(block)], there, x_send.at[way, block], x_recv.at[way, block], near[way]
        )

    def x_second(block, way):
        owner = left if way == 0 else right
        there = rows_all.at[owner, span_of(block, way * half, half)]
        return remote(
            there, there, x_send.at[2 + way, block], x_recv.at[2 + way, block], near[way]
        )

    def t_first(block, way):
        there = terms_all.at[me, group_of(block)]
        return remote(there, there, h_send.at[way, block], h_recv.at[way, block], near[way])

    def t_second(block, way):
        owner = left if way == 0 else right
        there = terms_all.at[owner, group_of(block, way * group // 2, group // 2)]
        return remote(
            there, there, h_send.at[2 + way, block], h_recv.at[2 + way, block], near[way]
        )

    full = tp_size * slice_width
    core_rows = shard_rows // 2
    piece_rows = core_rows // z_size
    piece_cols = full // x_size

    def w_piece(z_at, x_at, start=0, size=piece_cols):
        first = pl.multiple_of(core * core_rows + z_at * piece_rows, piece_rows)
        return (
            pl.ds(first, piece_rows),
            pl.ds(pl.multiple_of(x_at * piece_cols + start, piece_cols // 2), size),
        )

    def w_column(x_at, start=0, size=piece_cols):
        return (
            pl.ds(pl.multiple_of(core * core_rows, core_rows), core_rows),
            pl.ds(pl.multiple_of(x_at * piece_cols + start, piece_cols // 2), size),
        )

    own_rows, own_cols = w_piece(z_here, x_here)
    w_cross = [
        remote(
            out_hbm.at[own_rows, own_cols],
            out_w.at[slot, own_rows, own_cols],
            w_send.at[n],
            w_recv.at[n],
            {"tp": other},
        )
        for n, (other, slot) in enumerate(zip(around, (2, 1, 3)))
    ]

    def w_ring(axis, here, size, region, send, recv):
        copies = []
        for step in range(size // 2):
            pair = []
            for way in (0, 1):
                owner = lax.rem(here + (size - step if way == 0 else step), size)
                last = 2 * (step + 1) == size
                half_cols = piece_cols // 2
                rows, cols = region(owner, way * half_cols, half_cols) if last else region(owner)
                there = out_w.at[pl.ds(1, tp_size - 1), rows, cols]
                onward = {axis: lax.rem(here + (1 if way == 0 else size - 1), size)}
                pair.append(remote(there, there, send.at[way, step], recv.at[way, step], onward))
            copies.append(pair)
        return copies

    w_z = w_ring(
        "seq_1", z_here, z_size, lambda at, *cut: w_piece(at, x_here, *cut), wz_send, wz_recv
    )
    w_x = w_ring("seq_0", x_here, x_size, w_column, wx_send, wx_recv)
    w_waves = [w_cross] + w_z + w_x
    half_out_w = out_w.at[pl.ds(1, tp_size - 1), pl.ds(pl.multiple_of(core * core_rows, core_rows), core_rows)]
    w_across = remote(half_out_w, half_out_w, w_send.at[3], w_recv.at[3], {"seq_2": 1 - core})

    def w_move(wave):
        for one in w_waves[wave]:
            one.wait_recv()
        for one in w_waves[wave + 1] if wave + 1 < len(w_waves) else [w_across]:
            one.start()

    def prepare(block):
        rows, cols = iotas(SPAN)
        ones = jnp.ones((SPAN, SPAN), F32)
        upper = jnp.where(rows <= cols, 1.0, 0.0)
        for h in range(heads):
            tokens = span_of(block)
            decay = jnp.broadcast_to(decay_ref[h : h + 1, tokens], (SPAN, SPAN))
            rate = jnp.broadcast_to(rate_ref[h : h + 1, tokens], (SPAN, SPAN))
            along = mm_exact(decay[0:8], upper)[0:1]
            total = mm_exact(decay[0:8], ones)[0:1]
            down = mm_exact(jnp.where(rows >= cols, decay, 0.0), ones)
            beta = mm_exact(jnp.where(rows == cols, rate, 0.0), ones)
            fade = jnp.where(rows >= cols, jnp.exp(jnp.minimum(down - along, 0.0)), 0.0)
            grown = jnp.exp(down)
            fade_of[h, tokens, :] = fade
            system_of[h, tokens, :] = jnp.where(rows > cols, beta * fade, 0.0)
            grown_of[h, tokens, :] = grown
            side_of[h, tokens, :] = beta * grown
            rate_of[h, tokens, :] = beta
            tail_of[h, tokens, :] = jnp.exp(total - down)
            total_of[h, block] = jnp.broadcast_to(jnp.exp(total), total_of.shape[2:])

    def project(block):
        tokens = group_of(block)
        spread = [rows_all[j, tokens, :].astype(F32) for j in range(tp_size)]
        squares = sum(jnp.sum(part * part, axis=1, keepdims=True) for part in spread)
        scale = lax.rsqrt(squares * (1.0 / (tp_size * slice_width)) + norm_floor)
        normed = jnp.concatenate(
            [
                (part * scale * attn_gain_ref[:, j * slice_width : (j + 1) * slice_width]).astype(
                    BF16
                )
                for j, part in enumerate(spread)
            ],
            axis=1,
        )
        return normed

    chains = [(c, h) for c in range(GROUP) for h in range(heads)]

    def cut(part):
        return [part[c * SPAN : (c + 1) * SPAN, h * width : (h + 1) * width] for c, h in chains]

    def recur(block):
        normed = project(block)
        spans = [span_of(block * GROUP + c) for c, h in chains]

        def stored(ref):
            return [ref[h, tokens, :] for (c, h), tokens in zip(chains, spans)]

        keys = [unit_rows(part) for part in cut(jnp.dot(normed, qkv_w[1], preferred_element_type=F32))]
        key_key = [mm(k, k, ((1,), (1,))) for k in keys]
        values = cut(jnp.dot(normed, qkv_w[2], preferred_element_type=F32))
        inverse = inverses([kk * f for kk, f in zip(key_key, stored(system_of))])
        sides = [
            jnp.concatenate([g * k, b * v], axis=1)
            for b, g, k, v in zip(stored(rate_of), stored(side_of), keys, values)
        ]
        solved = [mm(x, s).astype(BF16) for x, s in zip(inverse, sides)]
        tails = [k * t for k, t in zip(keys, stored(tail_of))]
        terms = [mm(k, s, ((0,), (0,))) for k, s in zip(tails, solved)]
        before = []
        for n, (c, h) in enumerate(chains):
            growth = growth_now[h][0:1]
            entry_terms = running[h]
            before.append((growth, entry_terms))
            step = total_of[h, block * GROUP + c][0:1]
            new_growth, new_terms = compose((growth, entry_terms), (step, terms[n]))
            running[h] = new_terms
            growth_now[h] = jnp.broadcast_to(new_growth, growth_now.shape[1:])
        return (block, spans, stored, normed, keys, solved, before)

    def query(known):
        block, spans, stored, normed, keys, solved, before = known
        queries = [unit_rows(part) for part in cut(jnp.dot(normed, qkv_w[0], preferred_element_type=F32))]
        query_key = [mm(q, k, ((1,), (1,))) for q, k in zip(queries, keys)]
        mixed = [mm(qk * f, s) for qk, f, s in zip(query_key, stored(fade_of), solved)]
        entries = [
            g * q - m[:, :width] for g, q, m in zip(stored(grown_of), queries, mixed)
        ]
        reached = [mm(e, b[1]) for e, b in zip(entries, before)]
        for n, ((c, h), tokens) in enumerate(zip(chains, spans)):
            local = mixed[n][:, width:] + reached[n][:, width:]
            onward = before[n][0] * entries[n] - reached[n][:, :width]
            terms_all[me, tokens, h * width : (h + 1) * width] = local.astype(BF16)
            terms_all[me, tokens, (heads + h) * width : (heads + h + 1) * width] = onward.astype(
                BF16
            )

    for block in range(min(AHEAD, blocks)):
        for way in (0, 1):
            x_first(block, way).start()
        if block == 0:
            for one in w_cross:
                one.start()
    rows_all[me] = x_ref[...]
    running[...] = jnp.zeros_like(running)
    growth_now[...] = jnp.ones_like(growth_now)

    @pl.loop(0, blocks)
    def _(block):
        prepare(block)

    loads[0].wait()
    w_move(0)

    slots = [(n, when) for n in range(groups) for when in (("early", "late") if n else ("early",))]
    plan = list(zip(range(1, len(w_waves) - 2), slots))
    early = [(wave, n) for wave, (n, when) in plan if when == "early"]
    late = [(wave, n) for wave, (n, when) in plan if when == "late"]

    @pl.loop(0, groups)
    def _(block):
        for part in range(GROUP):
            now = block * GROUP + part
            for way in (0, 1):
                x_first(now, way).wait_recv()
                x_second(now, way).start()

            @pl.when(now + AHEAD < blocks)
            def _(now=now):
                for way in (0, 1):
                    x_first(now + AHEAD, way).start()

        for wave, at in early:

            @pl.when(block == at)
            def _(wave=wave):
                w_move(wave)

        @pl.when(block > 0)
        def _():
            for part in range(GROUP):
                for way in (0, 1):
                    x_second((block - 1) * GROUP + part, way).wait_recv()
            query(recur(block - 1))

        for wave, at in late:

            @pl.when(block == at)
            def _(wave=wave):
                w_move(wave)

    for block in range(groups - 1):
        for way in (0, 1):
            t_first(block, way).start()
    for block in range(blocks - GROUP, blocks):
        for way in (0, 1):
            x_second(block, way).wait_recv()
    last = recur(groups - 1)
    w_left = len(w_waves) - 1 - len(early) - len(late)
    for wave in range(len(w_waves) - w_left, len(w_waves) - 1):
        w_move(wave)

    partner = {"seq_2": 1 - core}
    for h in range(heads):
        keep(pair_mine.at[h], (growth_now[h][0:1], running[h]))
    pair_copy = remote(pair_mine, pair_other, pair_send.at[0], pair_recv.at[0], partner)
    pair_copy.start()
    pair_copy.wait_recv()
    own, other = (unpacked(pair_mine.at[core]), unpacked(pair_other.at[core]))
    chip = compose(choose(core == 0, own, other), choose(core == 0, other, own))
    keep(z_held.at[z_here], chip)
    nothing = (jnp.ones((1, width), F32), jnp.zeros((width, 2 * width), F32))
    sums = {"before": [nothing, nothing], "after": [nothing, nothing]}

    def t_pass(block):
        for way in (0, 1):
            t_first(block, way).wait_recv()
            t_second(block, way).start()

    def z_arrived(step, ways):
        if step < 0:
            query(last)
            for way in (0, 1):
                t_first(groups - 1, way).start()
        if 0 < step < groups:
            t_pass(step - 1)
        for way in ways:
            earlier = z_here > step if way == 0 else z_here + 1 + step >= z_size
            owner = lax.rem(z_here + (z_size - 1 - step if way == 0 else 1 + step), z_size)
            item = unpacked(z_held.at[owner])
            so_far = choose(earlier, sums["before"][way], sums["after"][way])
            joint = compose(item, so_far) if way == 0 else compose(so_far, item)
            sums["before"][way] = choose(earlier, joint, sums["before"][way])
            sums["after"][way] = choose(earlier, sums["after"][way], joint)

    ring_copies = ring_gather("seq_1", z_size, z_held, z_send, z_recv, z_arrived)
    through = compose(sums["before"][1], sums["before"][0])
    rest = compose(sums["after"][1], sums["after"][0])
    keep(x_held.at[x_here], compose(compose(through, chip), rest))

    def x_arrived(step, ways):
        if step < 0:
            w_move(len(w_waves) - 1)
            for block in range(max(0, min(groups, z_size // 2) - 1), groups - 1):
                t_pass(block)
        if step == 0:
            t_pass(groups - 1)

    ring_copies += ring_gather("seq_0", x_size, x_held, s_send, s_recv, x_arrived)
    chosen = jnp.zeros((width, width), F32)
    for back in range(x_size - 1, 0, -1):
        owner = lax.rem(x_here + x_size - back, x_size)
        chosen = jnp.where(x_here >= back, apply_terms(unpacked(x_held.at[owner]), chosen), chosen)
    first_terms = choose(core == 0, own, other)
    reached = apply_terms(through, chosen)
    leaving[0] = reached.astype(BF16)
    leaving[1] = apply_terms(first_terms, reached).astype(BF16)
    states[me, core] = leaving[core]
    state_copies = []
    for n, device in enumerate(friends[:7]):
        there = core if n < 3 else 1 - core
        state_copies.append(
            remote(leaving.at[there], states.at[me, core], st_send.at[n], st_recv.at[n], device)
        )
    for n in (2, 6, 0, 1, 3, 4, 5):
        state_copies[n].start()
    for load in loads[1:]:
        load.wait()
    w_across.wait_recv()
    for block in range(groups):
        for way in (0, 1):
            t_second(block, way).wait_recv()
    for n, (origin, head) in enumerate(
        [(left, core), (right, core), (opposite, core)]
        + [(me, 1 - core)]
        + [(left, 1 - core), (right, 1 - core), (opposite, 1 - core)]
    ):
        remote(
            leaving.at[0], states.at[origin, head], st_send.at[n], st_recv.at[n], {"tp": right}
        ).wait_recv()

    def r_far(block, way):
        return remote(
            parts.at[block, opposite, pl.ds(way * half, half)],
            passing.at[way, block],
            r_send.at[way, block],
            r_recv.at[way, block],
            near[way],
        )

    def r_direct(block, way):
        target = right if way == 0 else left
        piece = pl.ds((1 - way) * half, half)
        return remote(
            parts.at[block, target, piece],
            landed.at[way, block, piece],
            r_send.at[2 + way, block],
            r_recv.at[2 + way, block],
            near[way],
        )

    def r_joined(block, way):
        return remote(
            joined.at[way, block],
            landed.at[way, block, pl.ds(way * half, half)],
            r_send.at[4 + way, block],
            r_recv.at[4 + way, block],
            near[way],
        )

    def feed_forward(block):
        outs = []
        for origin in (me, *around):
            for h in range(heads):
                local = terms_all[origin, span_of(block), h * width : (h + 1) * width]
                onward = terms_all[
                    origin, span_of(block), (heads + h) * width : (heads + h + 1) * width
                ]
                raw = local.astype(F32) + mm(onward, states[origin, h])
                level = jnp.mean(raw * raw, axis=-1, keepdims=True)
                outs.append((raw * lax.rsqrt(level + head_floor) * head_gain_ref[...]).astype(BF16))
        attended = jnp.concatenate(outs, axis=1)
        squares = jnp.zeros((SPAN, 1), F32)
        for j in range(tp_size):
            piece = rows_all[j, span_of(block), :].astype(F32) + jnp.dot(
                attended,
                out_w[:, :, j * slice_width : (j + 1) * slice_width].reshape(
                    tp_size * shard_rows, slice_width
                ),
                preferred_element_type=F32,
            )
            resid[j] = piece
            squares = squares + jnp.sum(piece * piece, axis=1, keepdims=True)
        scale = lax.rsqrt(squares * (1.0 / (tp_size * slice_width)) + norm_floor)
        normed = jnp.concatenate(
            [
                (
                    resid[j] * scale * ffn_gain_ref[:, j * slice_width : (j + 1) * slice_width]
                ).astype(BF16)
                for j in range(tp_size)
            ],
            axis=1,
        )
        kept[span_of(block), :] = resid[me]
        gate_act = jnp.dot(normed, gate_w[...], preferred_element_type=F32)
        up_act = jnp.dot(normed, up_w[...], preferred_element_type=F32)
        hidden = (jax.nn.silu(gate_act) * up_act).astype(BF16)
        for j in range(tp_size):
            parts[block, j] = jnp.dot(
                hidden,
                down_w[:, j * slice_width : (j + 1) * slice_width],
                preferred_element_type=F32,
            ).astype(BF16)

    def join(block):
        for way in (0, 1):
            r_far(block, way).wait_recv()
            target = right if way == 0 else left
            joined[way, block] = (
                passing[way, block].astype(F32)
                + parts[block, target, pl.ds(way * half, half), :].astype(F32)
            ).astype(BF16)
            r_joined(block, way).start()

    def finish(block):
        for way in (0, 1):
            r_direct(block, way).wait_recv()
            r_joined(block, way).wait_recv()
        total = kept[span_of(block), :] + parts[block, me].astype(F32)
        total = total + landed[0, block].astype(F32) + landed[1, block].astype(F32)
        o_ref[span_of(block), :] = total.astype(BF16)

    @pl.loop(0, blocks + 2)
    def _(block):
        @pl.when(block < blocks)
        def _():
            feed_forward(block)
            for way in (0, 1):
                r_far(block, way).start()
                r_direct(block, way).start()

        @pl.when((block > 0) & (block < blocks + 1))
        def _():
            join(block - 1)

        @pl.when(block > 1)
        def _():
            finish(block - 2)

    @pl.loop(0, blocks)
    def _(block):
        for way in (0, 1):
            x_first(block, way).wait_send()
            x_second(block, way).wait_send()
            r_far(block, way).wait_send()
            r_direct(block, way).wait_send()
            r_joined(block, way).wait_send()

    @pl.loop(0, groups)
    def _(block):
        for way in (0, 1):
            t_first(block, way).wait_send()
            t_second(block, way).wait_send()

    w_copies = [one for wave in w_waves for one in wave] + [w_across]
    for one in w_copies + state_copies + [pair_copy] + ring_copies:
        one.wait_send()


def body(
    sizes,
    layer_in,
    attn_gain,
    qkv_weight,
    log_decay,
    write_rate,
    head_gain,
    out_weight,
    ffn_gain,
    gate_weight,
    up_weight,
    down_weight,
):
    x_size, z_size, tp_size = sizes
    length, slice_width = layer_in.shape
    full = tp_size * slice_width
    width = head_gain.shape[0]
    heads = qkv_weight.shape[2] // width
    blocks = length // SPAN
    hidden = gate_weight.shape[1]
    shard_rows = out_weight.shape[0]

    vmem = pl.BlockSpec(memory_space=pltpu.VMEM)
    anywhere = pl.BlockSpec(memory_space=pl.ANY)
    dma = pltpu.SemaphoreType.DMA
    scratch = [
        pltpu.VMEM(qkv_weight.shape, BF16),
        pltpu.VMEM((tp_size, shard_rows, full), BF16),
        pltpu.VMEM(gate_weight.shape, BF16),
        pltpu.VMEM(up_weight.shape, BF16),
        pltpu.VMEM(down_weight.shape, BF16),
        pltpu.VMEM((tp_size, length, slice_width), BF16),
        pltpu.VMEM((tp_size, length, 2 * heads * width), BF16),
        pltpu.VMEM((heads, width, 2 * width), F32),
        pltpu.VMEM((heads, 8, width), F32),
        *[pltpu.VMEM((heads, length, SPAN), F32) for _ in range(6)],
        pltpu.VMEM((heads, blocks, 8, width), F32),
        pltpu.VMEM((heads, 2, width + 16, width), BF16),
        pltpu.VMEM((heads, 2, width + 16, width), BF16),
        pltpu.VMEM((z_size, 2, width + 16, width), BF16),
        pltpu.VMEM((x_size, 2, width + 16, width), BF16),
        pltpu.VMEM((tp_size, heads, width, width), BF16),
        pltpu.VMEM((2, width, width), BF16),
        pltpu.VMEM((blocks, tp_size, SPAN, slice_width), BF16),
        pltpu.VMEM((2, blocks, SPAN // 2, slice_width), BF16),
        pltpu.VMEM((2, blocks, SPAN // 2, slice_width), BF16),
        pltpu.VMEM((2, blocks, SPAN, slice_width), BF16),
        pltpu.VMEM((tp_size, SPAN, slice_width), F32),
        pltpu.VMEM((length, slice_width), F32),
        dma((5,)),
        dma((4, blocks)),
        dma((4, blocks)),
        dma((4, blocks // GROUP)),
        dma((4, blocks // GROUP)),
        dma((6, blocks)),
        dma((6, blocks)),
        dma((4,)),
        dma((4,)),
        dma((2, z_size // 2)),
        dma((2, z_size // 2)),
        dma((2, x_size // 2)),
        dma((2, x_size // 2)),
        dma((7,)),
        dma((7,)),
        dma((2,)),
        dma((2,)),
        dma((2, 2, z_size)),
        dma((2, 2, z_size)),
        dma((2, 2, x_size)),
        dma((2, 2, x_size)),
    ]
    return pl.pallas_call(
        functools.partial(layer_kernel, (x_size, z_size, tp_size, blocks)),
        out_shape=jax.ShapeDtypeStruct((length, slice_width), BF16),
        in_specs=[vmem] * 6 + [anywhere] * 5,
        out_specs=vmem,
        scratch_shapes=scratch,
        compiler_params=pltpu.CompilerParams(
            collective_id=0, has_side_effects=True, vmem_limit_bytes=60 * 1024 * 1024
        ),
        name="layer",
    )(
        layer_in,
        attn_gain.reshape(1, full),
        log_decay,
        write_rate,
        head_gain.reshape(1, width),
        ffn_gain.reshape(1, full),
        qkv_weight,
        out_weight,
        gate_weight,
        up_weight,
        down_weight,
    )


def layer(shape, tp_size):
    x_size, z_size, cores = shape
    in_specs = (
        P(SEQ, "tp"),
        P(),
        P(None, None, "tp"),
        P("tp", SEQ),
        P("tp", SEQ),
        P(),
        P("tp", None),
        P(),
        P(None, "tp"),
        P(None, "tp"),
        P("tp", None),
    )
    return functools.partial(body, (x_size, z_size, tp_size)), in_specs, P(SEQ, "tp")


def solution(mesh):
    torus = Mesh(mesh.devices.reshape(4, 8, 2, mesh.shape["tp"]), (*SEQ, "tp"))
    function, in_specs, out_specs = layer((4, 8, 2), mesh.shape["tp"])
    return jax.shard_map(
        function, mesh=torus, in_specs=in_specs, out_specs=out_specs, check_vma=False
    )
```

```python
import functools

import jax
import jax.numpy as jnp
from jax import lax
from jax.experimental import pallas as pl
from jax.experimental.pallas import tpu as pltpu
from jax.sharding import Mesh
from jax.sharding import PartitionSpec as P

SEQ = ("seq_0", "seq_1", "seq_2")
MESH = pl.DeviceIdType.MESH
BF16 = jnp.bfloat16
F32 = jnp.float32

norm_floor = 0.1
head_floor = 0.05
SPAN = 128
GROUP = 2
AHEAD = 3


def mm(a, b, dims=((1,), (0,))):
    return lax.dot_general(
        a.astype(BF16), b.astype(BF16), (dims, ((), ())), preferred_element_type=F32
    )


def mm_exact(a, b):
    return lax.dot_general(
        a, b, (((1,), (0,)), ((), ())), preferred_element_type=F32, precision=lax.Precision.HIGHEST
    )


def unit_rows(vectors):
    return vectors * lax.rsqrt(jnp.sum(vectors * vectors, axis=-1, keepdims=True) + 1.0)


def iotas(size):
    rows = lax.broadcasted_iota(jnp.int32, (size, size), 0)
    cols = lax.broadcasted_iota(jnp.int32, (size, size), 1)
    return (rows, cols)


def inverses(lowers):
    size = lowers[0].shape[0]
    rows, cols = iotas(size)
    pairs = rows // 2 == cols // 2
    found = [jnp.where(rows == cols, 1.0, jnp.where(pairs, -a, 0.0)) for a in lowers]
    block = 2
    while block < size:
        wide = min(4 * block, size)
        pick = (rows // wide == cols // wide) & (rows // block != cols // block)
        inner = [mm(x, jnp.where(pick, a, 0.0)) for a, x in zip(lowers, found)]
        near = [x - mm(n, x) for n, x in zip(inner, found)]
        twice = [mm(n, n) for n in inner]
        found = [x + mm(n, x) for n, x in zip(twice, near)]
        block *= 4
    return found


def compose(earlier, later):
    first_growth, first = earlier
    second_growth, second = later
    width = first.shape[0]
    second_map = second[:, :width]
    both_growth = jnp.concatenate([second_growth, second_growth], axis=1)
    own = jnp.concatenate([first_growth * second_map, second[:, width:]], axis=1)
    return (first_growth * second_growth, both_growth * first + own - mm(second_map, first))


def apply_terms(terms, state):
    growth, both = terms
    width = both.shape[0]
    return growth * state - mm(both[:, :width], state) + both[:, width:]


def packed(terms):
    growth, both = terms
    high = growth.astype(BF16).astype(F32)
    middle = (growth - high).astype(BF16).astype(F32)
    low = growth - high - middle
    width = both.shape[0]
    row = lax.broadcasted_iota(jnp.int32, (16, width), 0)
    parts = jnp.where(row == 0, high, jnp.where(row == 1, middle, jnp.where(row == 2, low, 0.0)))
    return jnp.concatenate([both[:, :width], parts], axis=0).astype(BF16), both[:, width:].astype(BF16)


def keep(message, terms):
    upper, lower = packed(terms)
    message[0] = upper
    message[1, pl.ds(0, lower.shape[0]), :] = lower


def unpacked(message):
    width = message.shape[2]
    upper = message[0].astype(F32)
    growth = upper[width : width + 1] + upper[width + 1 : width + 2] + upper[width + 2 : width + 3]
    lower = message[1, pl.ds(0, width), :].astype(F32)
    return (growth, jnp.concatenate([upper[:width], lower], axis=1))


def choose(first, terms, others):
    return tuple(jnp.where(first, a, b) for a, b in zip(terms, others))


def ring_gather(axis, size, held, send_sem, recv_sem, arrived):
    here = lax.axis_index(axis)
    right, left = (lax.rem(here + 1, size), lax.rem(here + size - 1, size))
    width = held.shape[3]

    def copy(way, step, part):
        owner = lax.rem(here + size - step, size) if way == 0 else lax.rem(here + step, size)
        piece = held.at[owner, part, pl.ds(0, width + 16 if part == 0 else width)]
        return pltpu.make_async_remote_copy(
            src_ref=piece,
            dst_ref=piece,
            send_sem=send_sem.at[way, part, step],
            recv_sem=recv_sem.at[way, part, step],
            device_id={axis: right if way == 0 else left},
            device_id_type=MESH,
        )

    steps = size // 2
    order = ((0, 1), (1, 0))
    copies = [
        [
            {
                part: copy(way, step, part)
                for part in order[way]
                if part == way or 2 * (step + 1) < size
            }
            for step in range(steps)
        ]
        for way in (0, 1)
    ]
    for n in (0, 1):
        for way in (0, 1):
            if order[way][n] in copies[way][0]:
                copies[way][0][order[way][n]].start()
    arrived(-1, ())
    for step in range(steps):
        for n in (0, 1):
            for way in (0, 1):
                part = order[way][n]
                if part in copies[way][step]:
                    copies[way][step][part].wait_recv()
                    if step + 1 < steps and part in copies[way][step + 1]:
                        copies[way][step + 1][part].start()
        arrived(step, (0, 1) if 2 * (step + 1) < size else (0,))
    return [one for way in copies for step in way for one in step.values()]


def layer_kernel(
    sizes,
    x_hbm,
    attn_gain_hbm,
    decay_hbm,
    rate_hbm,
    head_gain_hbm,
    ffn_gain_hbm,
    qkv_hbm,
    out_hbm,
    gate_hbm,
    up_hbm,
    down_hbm,
    o_ref,
    attn_gain_ref,
    decay_ref,
    rate_ref,
    head_gain_ref,
    ffn_gain_ref,
    qkv_w,
    out_w,
    gate_w,
    up_w,
    down_w,
    rows_all,
    terms_all,
    running,
    growth_now,
    fade_of,
    system_of,
    grown_of,
    side_of,
    rate_of,
    tail_of,
    total_of,
    pair_mine,
    pair_other,
    z_held,
    x_held,
    states,
    leaving,
    parts,
    passing,
    joined,
    landed,
    resid,
    kept,
    load_sem,
    x_send,
    x_recv,
    h_send,
    h_recv,
    r_send,
    r_recv,
    w_send,
    w_recv,
    wz_send,
    wz_recv,
    wx_send,
    wx_recv,
    st_send,
    st_recv,
    pair_send,
    pair_recv,
    z_send,
    z_recv,
    s_send,
    s_recv,
):
    x_size, z_size, tp_size, blocks = sizes
    me = lax.axis_index("tp")
    core = lax.axis_index("seq_2")
    z_here = lax.axis_index("seq_1")
    x_here = lax.axis_index("seq_0")
    right, left = (lax.rem(me + 1, tp_size), lax.rem(me + tp_size - 1, tp_size))
    opposite = lax.rem(me + 2, tp_size)
    width = head_gain_ref.shape[1]
    heads = decay_ref.shape[0]
    slice_width = x_hbm.shape[1]
    shard_rows = heads * width
    half = SPAN // 2
    near = {"tp": right}, {"tp": left}

    loads = [
        pltpu.make_async_copy(qkv_hbm, qkv_w, load_sem.at[0]),
        pltpu.make_async_copy(out_hbm, out_w.at[0], load_sem.at[1]),
        pltpu.make_async_copy(gate_hbm, gate_w, load_sem.at[2]),
        pltpu.make_async_copy(up_hbm, up_w, load_sem.at[3]),
        pltpu.make_async_copy(down_hbm, down_w, load_sem.at[4]),
    ]
    early_loads = [
        pltpu.make_async_copy(source, target, load_sem.at[5 + n])
        for n, (source, target) in enumerate(
            (
                (x_hbm, rows_all.at[me]),
                (decay_hbm, decay_ref),
                (rate_hbm, rate_ref),
                (attn_gain_hbm, attn_gain_ref),
                (head_gain_hbm, head_gain_ref),
                (ffn_gain_hbm, ffn_gain_ref),
            )
        )
    ]
    for load in early_loads:
        load.start()
    barrier = pltpu.get_barrier_semaphore()
    around = (right, left, opposite)
    friends = [{"tp": other} for other in around] + [{"seq_2": 1 - core}]
    friends += [{"tp": other, "seq_2": 1 - core} for other in around]
    for axis, here, size in (("seq_1", z_here, z_size), ("seq_0", x_here, x_size)):
        friends.append({axis: lax.rem(here + 1, size)})
        friends.append({axis: lax.rem(here + size - 1, size)})
    for friend in friends:
        pl.semaphore_signal(barrier, inc=1, device_id=friend, device_id_type=MESH)
    for load in loads:
        load.start()
    early_loads[0].wait()
    pl.semaphore_wait(barrier, len(friends))

    def span_of(block, start=0, size=SPAN):
        return pl.ds(pl.multiple_of(block * SPAN + start, half), size)

    def remote(source, target, send, recv, device):
        return pltpu.make_async_remote_copy(
            src_ref=source,
            dst_ref=target,
            send_sem=send,
            recv_sem=recv,
            device_id=device,
            device_id_type=MESH,
        )

    group = GROUP * SPAN
    groups = blocks // GROUP

    def group_of(block, start=0, size=group):
        return pl.ds(pl.multiple_of(block * group + start, half), size)

    def x_first(block, way):
        there = rows_all.at[me, span_of(block)]
        return remote(there, there, x_send.at[way, block], x_recv.at[way, block], near[way])

    def x_second(block, way):
        owner = left if way == 0 else right
        there = rows_all.at[owner, span_of(block, way * half, half)]
        return remote(
            there, there, x_send.at[2 + way, block], x_recv.at[2 + way, block], near[way]
        )

    def t_first(block, way):
        there = terms_all.at[me, group_of(block)]
        return remote(there, there, h_send.at[way, block], h_recv.at[way, block], near[way])

    def t_second(block, way):
        owner = left if way == 0 else right
        there = terms_all.at[owner, group_of(block, way * group // 2, group // 2)]
        return remote(
            there, there, h_send.at[2 + way, block], h_recv.at[2 + way, block], near[way]
        )

    full = tp_size * slice_width
    core_rows = shard_rows // 2
    piece_rows = core_rows // z_size
    piece_cols = full // x_size

    def w_piece(z_at, x_at, start=0, size=piece_cols):
        first = pl.multiple_of(core * core_rows + z_at * piece_rows, piece_rows)
        return (
            pl.ds(first, piece_rows),
            pl.ds(pl.multiple_of(x_at * piece_cols + start, piece_cols // 2), size),
        )

    def w_column(x_at, start=0, size=piece_cols):
        return (
            pl.ds(pl.multiple_of(core * core_rows, core_rows), core_rows),
            pl.ds(pl.multiple_of(x_at * piece_cols + start, piece_cols // 2), size),
        )

    own_rows, own_cols = w_piece(z_here, x_here)
    w_cross = [
        remote(
            out_hbm.at[own_rows, own_cols],
            out_w.at[slot, own_rows, own_cols],
            w_send.at[n],
            w_recv.at[n],
            {"tp": other},
        )
        for n, (other, slot) in enumerate(zip(around, (2, 1, 3)))
    ]

    def w_ring(axis, here, size, region, send, recv):
        copies = []
        for step in range(size // 2):
            pair = []
            for way in (0, 1):
                owner = lax.rem(here + (size - step if way == 0 else step), size)
                last = 2 * (step + 1) == size
                half_cols = piece_cols // 2
                rows, cols = region(owner, way * half_cols, half_cols) if last else region(owner)
                there = out_w.at[pl.ds(1, tp_size - 1), rows, cols]
                onward = {axis: lax.rem(here + (1 if way == 0 else size - 1), size)}
                pair.append(remote(there, there, send.at[way, step], recv.at[way, step], onward))
            copies.append(pair)
        return copies

    w_z = w_ring(
        "seq_1", z_here, z_size, lambda at, *cut: w_piece(at, x_here, *cut), wz_send, wz_recv
    )
    w_x = w_ring("seq_0", x_here, x_size, w_column, wx_send, wx_recv)
    w_waves = [w_cross] + w_z + w_x
    half_out_w = out_w.at[pl.ds(1, tp_size - 1), pl.ds(pl.multiple_of(core * core_rows, core_rows), core_rows)]
    w_across = remote(half_out_w, half_out_w, w_send.at[3], w_recv.at[3], {"seq_2": 1 - core})

    def w_move(wave):
        for one in w_waves[wave]:
            one.wait_recv()
        for one in w_waves[wave + 1] if wave + 1 < len(w_waves) else [w_across]:
            one.start()

    def prepare(block):
        rows, cols = iotas(SPAN)
        ones = jnp.ones((SPAN, SPAN), F32)
        upper = jnp.where(rows <= cols, 1.0, 0.0)
        for h in range(heads):
            tokens = span_of(block)
            decay = jnp.broadcast_to(decay_ref[h : h + 1, tokens], (SPAN, SPAN))
            rate = jnp.broadcast_to(rate_ref[h : h + 1, tokens], (SPAN, SPAN))
            along = mm_exact(decay[0:8], upper)[0:1]
            total = mm_exact(decay[0:8], ones)[0:1]
            down = mm_exact(jnp.where(rows >= cols, decay, 0.0), ones)
            beta = mm_exact(jnp.where(rows == cols, rate, 0.0), ones)
            fade = jnp.where(rows >= cols, jnp.exp(jnp.minimum(down - along, 0.0)), 0.0)
            grown = jnp.exp(down)
            fade_of[h, tokens, :] = fade
            system_of[h, tokens, :] = jnp.where(rows > cols, beta * fade, 0.0)
            grown_of[h, tokens, :] = grown
            side_of[h, tokens, :] = beta * grown
            rate_of[h, tokens, :] = beta
            tail_of[h, tokens, :] = jnp.exp(total - down)
            total_of[h, block] = jnp.broadcast_to(jnp.exp(total), total_of.shape[2:])

    def project(block):
        tokens = group_of(block)
        spread = [rows_all[j, tokens, :].astype(F32) for j in range(tp_size)]
        squares = sum(jnp.sum(part * part, axis=1, keepdims=True) for part in spread)
        scale = lax.rsqrt(squares * (1.0 / (tp_size * slice_width)) + norm_floor)
        normed = jnp.concatenate(
            [
                (part * scale * attn_gain_ref[:, j * slice_width : (j + 1) * slice_width]).astype(
                    BF16
                )
                for j, part in enumerate(spread)
            ],
            axis=1,
        )
        return normed

    chains = [(c, h) for c in range(GROUP) for h in range(heads)]

    def cut(part):
        return [part[c * SPAN : (c + 1) * SPAN, h * width : (h + 1) * width] for c, h in chains]

    def recur(block):
        normed = project(block)
        spans = [span_of(block * GROUP + c) for c, h in chains]

        def stored(ref):
            return [ref[h, tokens, :] for (c, h), tokens in zip(chains, spans)]

        keys = [unit_rows(part) for part in cut(jnp.dot(normed, qkv_w[1], preferred_element_type=F32))]
        key_key = [mm(k, k, ((1,), (1,))) for k in keys]
        values = cut(jnp.dot(normed, qkv_w[2], preferred_element_type=F32))
        inverse = inverses([kk * f for kk, f in zip(key_key, stored(system_of))])
        sides = [
            jnp.concatenate([g * k, b * v], axis=1)
            for b, g, k, v in zip(stored(rate_of), stored(side_of), keys, values)
        ]
        solved = [mm(x, s).astype(BF16) for x, s in zip(inverse, sides)]
        tails = [k * t for k, t in zip(keys, stored(tail_of))]
        terms = [mm(k, s, ((0,), (0,))) for k, s in zip(tails, solved)]
        before = []
        for n, (c, h) in enumerate(chains):
            growth = growth_now[h][0:1]
            entry_terms = running[h]
            before.append((growth, entry_terms))
            step = total_of[h, block * GROUP + c][0:1]
            new_growth, new_terms = compose((growth, entry_terms), (step, terms[n]))
            running[h] = new_terms
            growth_now[h] = jnp.broadcast_to(new_growth, growth_now.shape[1:])
        return (block, spans, stored, normed, keys, solved, before)

    def query(known):
        block, spans, stored, normed, keys, solved, before = known
        queries = [unit_rows(part) for part in cut(jnp.dot(normed, qkv_w[0], preferred_element_type=F32))]
        query_key = [mm(q, k, ((1,), (1,))) for q, k in zip(queries, keys)]
        mixed = [mm(qk * f, s) for qk, f, s in zip(query_key, stored(fade_of), solved)]
        entries = [
            g * q - m[:, :width] for g, q, m in zip(stored(grown_of), queries, mixed)
        ]
        reached = [mm(e, b[1]) for e, b in zip(entries, before)]
        for n, ((c, h), tokens) in enumerate(zip(chains, spans)):
            local = mixed[n][:, width:] + reached[n][:, width:]
            onward = before[n][0] * entries[n] - reached[n][:, :width]
            terms_all[me, tokens, h * width : (h + 1) * width] = local.astype(BF16)
            terms_all[me, tokens, (heads + h) * width : (heads + h + 1) * width] = onward.astype(
                BF16
            )

    for block in range(min(AHEAD, blocks)):
        for way in (0, 1):
            x_first(block, way).start()
        if block == 0:
            for one in w_cross:
                one.start()
    running[...] = jnp.zeros_like(running)
    growth_now[...] = jnp.ones_like(growth_now)

    for load in early_loads[1:]:
        load.wait()

    @pl.loop(0, blocks)
    def _(block):
        prepare(block)

    loads[0].wait()
    w_move(0)

    slots = [(n, when) for n in range(groups) for when in (("early", "late") if n else ("early",))]
    plan = list(zip(range(1, len(w_waves) - 2), slots))
    early = [(wave, n) for wave, (n, when) in plan if when == "early"]
    late = [(wave, n) for wave, (n, when) in plan if when == "late"]

    @pl.loop(0, groups)
    def _(block):
        for part in range(GROUP):
            now = block * GROUP + part
            for way in (0, 1):
                x_first(now, way).wait_recv()
                x_second(now, way).start()

            @pl.when(now + AHEAD < blocks)
            def _(now=now):
                for way in (0, 1):
                    x_first(now + AHEAD, way).start()

        for wave, at in early:

            @pl.when(block == at)
            def _(wave=wave):
                w_move(wave)

        @pl.when(block > 0)
        def _():
            for part in range(GROUP):
                for way in (0, 1):
                    x_second((block - 1) * GROUP + part, way).wait_recv()
            query(recur(block - 1))

        for wave, at in late:

            @pl.when(block == at)
            def _(wave=wave):
                w_move(wave)

    for block in range(groups - 1):
        for way in (0, 1):
            t_first(block, way).start()
    for block in range(blocks - GROUP, blocks):
        for way in (0, 1):
            x_second(block, way).wait_recv()
    last = recur(groups - 1)
    w_left = len(w_waves) - 1 - len(early) - len(late)
    for wave in range(len(w_waves) - w_left, len(w_waves) - 1):
        w_move(wave)

    partner = {"seq_2": 1 - core}
    for h in range(heads):
        keep(pair_mine.at[h], (growth_now[h][0:1], running[h]))
    pair_copy = remote(pair_mine, pair_other, pair_send.at[0], pair_recv.at[0], partner)
    pair_copy.start()
    pair_copy.wait_recv()
    own, other = (unpacked(pair_mine.at[core]), unpacked(pair_other.at[core]))
    chip = compose(choose(core == 0, own, other), choose(core == 0, other, own))
    keep(z_held.at[z_here], chip)
    nothing = (jnp.ones((1, width), F32), jnp.zeros((width, 2 * width), F32))
    sums = {"before": [nothing, nothing], "after": [nothing, nothing]}

    def t_pass(block):
        for way in (0, 1):
            t_first(block, way).wait_recv()
            t_second(block, way).start()

    def z_arrived(step, ways):
        if step < 0:
            query(last)
            for way in (0, 1):
                t_first(groups - 1, way).start()
        if 0 < step < groups:
            t_pass(step - 1)
        for way in ways:
            earlier = z_here > step if way == 0 else z_here + 1 + step >= z_size
            owner = lax.rem(z_here + (z_size - 1 - step if way == 0 else 1 + step), z_size)
            item = unpacked(z_held.at[owner])
            so_far = choose(earlier, sums["before"][way], sums["after"][way])
            joint = compose(item, so_far) if way == 0 else compose(so_far, item)
            sums["before"][way] = choose(earlier, joint, sums["before"][way])
            sums["after"][way] = choose(earlier, sums["after"][way], joint)

    ring_copies = ring_gather("seq_1", z_size, z_held, z_send, z_recv, z_arrived)
    through = compose(sums["before"][1], sums["before"][0])
    rest = compose(sums["after"][1], sums["after"][0])
    keep(x_held.at[x_here], compose(compose(through, chip), rest))

    def x_arrived(step, ways):
        if step < 0:
            w_move(len(w_waves) - 1)
            for block in range(max(0, min(groups, z_size // 2) - 1), groups - 1):
                t_pass(block)
        if step == 0:
            t_pass(groups - 1)

    ring_copies += ring_gather("seq_0", x_size, x_held, s_send, s_recv, x_arrived)
    chosen = jnp.zeros((width, width), F32)
    for back in range(x_size - 1, 0, -1):
        owner = lax.rem(x_here + x_size - back, x_size)
        chosen = jnp.where(x_here >= back, apply_terms(unpacked(x_held.at[owner]), chosen), chosen)
    first_terms = choose(core == 0, own, other)
    reached = apply_terms(through, chosen)
    leaving[0] = reached.astype(BF16)
    leaving[1] = apply_terms(first_terms, reached).astype(BF16)
    states[me, core] = leaving[core]
    state_copies = []
    for n, device in enumerate(friends[:7]):
        there = core if n < 3 else 1 - core
        state_copies.append(
            remote(leaving.at[there], states.at[me, core], st_send.at[n], st_recv.at[n], device)
        )
    for n in (2, 6, 0, 1, 3, 4, 5):
        state_copies[n].start()
    for load in loads[1:]:
        load.wait()
    w_across.wait_recv()
    for block in range(groups):
        for way in (0, 1):
            t_second(block, way).wait_recv()
    for n, (origin, head) in enumerate(
        [(left, core), (right, core), (opposite, core)]
        + [(me, 1 - core)]
        + [(left, 1 - core), (right, 1 - core), (opposite, 1 - core)]
    ):
        remote(
            leaving.at[0], states.at[origin, head], st_send.at[n], st_recv.at[n], {"tp": right}
        ).wait_recv()

    def r_far(block, way):
        return remote(
            parts.at[block, opposite, pl.ds(way * half, half)],
            passing.at[way, block],
            r_send.at[way, block],
            r_recv.at[way, block],
            near[way],
        )

    def r_direct(block, way):
        target = right if way == 0 else left
        piece = pl.ds((1 - way) * half, half)
        return remote(
            parts.at[block, target, piece],
            landed.at[way, block, piece],
            r_send.at[2 + way, block],
            r_recv.at[2 + way, block],
            near[way],
        )

    def r_joined(block, way):
        return remote(
            joined.at[way, block],
            landed.at[way, block, pl.ds(way * half, half)],
            r_send.at[4 + way, block],
            r_recv.at[4 + way, block],
            near[way],
        )

    def feed_forward(block):
        outs = []
        for origin in (me, *around):
            for h in range(heads):
                local = terms_all[origin, span_of(block), h * width : (h + 1) * width]
                onward = terms_all[
                    origin, span_of(block), (heads + h) * width : (heads + h + 1) * width
                ]
                raw = local.astype(F32) + mm(onward, states[origin, h])
                level = jnp.mean(raw * raw, axis=-1, keepdims=True)
                outs.append((raw * lax.rsqrt(level + head_floor) * head_gain_ref[...]).astype(BF16))
        attended = jnp.concatenate(outs, axis=1)
        squares = jnp.zeros((SPAN, 1), F32)
        for j in range(tp_size):
            piece = rows_all[j, span_of(block), :].astype(F32) + jnp.dot(
                attended,
                out_w[:, :, j * slice_width : (j + 1) * slice_width].reshape(
                    tp_size * shard_rows, slice_width
                ),
                preferred_element_type=F32,
            )
            resid[j] = piece
            squares = squares + jnp.sum(piece * piece, axis=1, keepdims=True)
        scale = lax.rsqrt(squares * (1.0 / (tp_size * slice_width)) + norm_floor)
        normed = jnp.concatenate(
            [
                (
                    resid[j] * scale * ffn_gain_ref[:, j * slice_width : (j + 1) * slice_width]
                ).astype(BF16)
                for j in range(tp_size)
            ],
            axis=1,
        )
        kept[span_of(block), :] = resid[me]
        gate_act = jnp.dot(normed, gate_w[...], preferred_element_type=F32)
        up_act = jnp.dot(normed, up_w[...], preferred_element_type=F32)
        hidden = (jax.nn.silu(gate_act) * up_act).astype(BF16)
        for j in range(tp_size):
            parts[block, j] = jnp.dot(
                hidden,
                down_w[:, j * slice_width : (j + 1) * slice_width],
                preferred_element_type=F32,
            ).astype(BF16)

    def join(block):
        for way in (0, 1):
            r_far(block, way).wait_recv()
            target = right if way == 0 else left
            joined[way, block] = (
                passing[way, block].astype(F32)
                + parts[block, target, pl.ds(way * half, half), :].astype(F32)
            ).astype(BF16)
            r_joined(block, way).start()

    def finish(block):
        for way in (0, 1):
            r_direct(block, way).wait_recv()
            r_joined(block, way).wait_recv()
        total = kept[span_of(block), :] + parts[block, me].astype(F32)
        total = total + landed[0, block].astype(F32) + landed[1, block].astype(F32)
        o_ref[span_of(block), :] = total.astype(BF16)

    @pl.loop(0, blocks + 2)
    def _(block):
        @pl.when(block < blocks)
        def _():
            feed_forward(block)
            for way in (0, 1):
                r_far(block, way).start()
                r_direct(block, way).start()

        @pl.when((block > 0) & (block < blocks + 1))
        def _():
            join(block - 1)

        @pl.when(block > 1)
        def _():
            finish(block - 2)

    @pl.loop(0, blocks)
    def _(block):
        for way in (0, 1):
            x_first(block, way).wait_send()
            x_second(block, way).wait_send()
            r_far(block, way).wait_send()
            r_direct(block, way).wait_send()
            r_joined(block, way).wait_send()

    @pl.loop(0, groups)
    def _(block):
        for way in (0, 1):
            t_first(block, way).wait_send()
            t_second(block, way).wait_send()

    w_copies = [one for wave in w_waves for one in wave] + [w_across]
    for one in w_copies + state_copies + [pair_copy] + ring_copies:
        one.wait_send()


def body(
    sizes,
    layer_in,
    attn_gain,
    qkv_weight,
    log_decay,
    write_rate,
    head_gain,
    out_weight,
    ffn_gain,
    gate_weight,
    up_weight,
    down_weight,
):
    x_size, z_size, tp_size = sizes
    length, slice_width = layer_in.shape
    full = tp_size * slice_width
    width = head_gain.shape[0]
    heads = qkv_weight.shape[2] // width
    blocks = length // SPAN
    hidden = gate_weight.shape[1]
    shard_rows = out_weight.shape[0]

    vmem = pl.BlockSpec(memory_space=pltpu.VMEM)
    anywhere = pl.BlockSpec(memory_space=pl.ANY)
    dma = pltpu.SemaphoreType.DMA
    scratch = [
        pltpu.VMEM((1, full), F32),
        pltpu.VMEM((heads, length), F32),
        pltpu.VMEM((heads, length), F32),
        pltpu.VMEM((1, width), F32),
        pltpu.VMEM((1, full), F32),
        pltpu.VMEM(qkv_weight.shape, BF16),
        pltpu.VMEM((tp_size, shard_rows, full), BF16),
        pltpu.VMEM(gate_weight.shape, BF16),
        pltpu.VMEM(up_weight.shape, BF16),
        pltpu.VMEM(down_weight.shape, BF16),
        pltpu.VMEM((tp_size, length, slice_width), BF16),
        pltpu.VMEM((tp_size, length, 2 * heads * width), BF16),
        pltpu.VMEM((heads, width, 2 * width), F32),
        pltpu.VMEM((heads, 8, width), F32),
        *[pltpu.VMEM((heads, length, SPAN), F32) for _ in range(6)],
        pltpu.VMEM((heads, blocks, 8, width), F32),
        pltpu.VMEM((heads, 2, width + 16, width), BF16),
        pltpu.VMEM((heads, 2, width + 16, width), BF16),
        pltpu.VMEM((z_size, 2, width + 16, width), BF16),
        pltpu.VMEM((x_size, 2, width + 16, width), BF16),
        pltpu.VMEM((tp_size, heads, width, width), BF16),
        pltpu.VMEM((2, width, width), BF16),
        pltpu.VMEM((blocks, tp_size, SPAN, slice_width), BF16),
        pltpu.VMEM((2, blocks, SPAN // 2, slice_width), BF16),
        pltpu.VMEM((2, blocks, SPAN // 2, slice_width), BF16),
        pltpu.VMEM((2, blocks, SPAN, slice_width), BF16),
        pltpu.VMEM((tp_size, SPAN, slice_width), F32),
        pltpu.VMEM((length, slice_width), F32),
        dma((11,)),
        dma((4, blocks)),
        dma((4, blocks)),
        dma((4, blocks // GROUP)),
        dma((4, blocks // GROUP)),
        dma((6, blocks)),
        dma((6, blocks)),
        dma((4,)),
        dma((4,)),
        dma((2, z_size // 2)),
        dma((2, z_size // 2)),
        dma((2, x_size // 2)),
        dma((2, x_size // 2)),
        dma((7,)),
        dma((7,)),
        dma((2,)),
        dma((2,)),
        dma((2, 2, z_size)),
        dma((2, 2, z_size)),
        dma((2, 2, x_size)),
        dma((2, 2, x_size)),
    ]
    return pl.pallas_call(
        functools.partial(layer_kernel, (x_size, z_size, tp_size, blocks)),
        out_shape=pltpu.VMEM((length, slice_width), BF16),
        in_specs=[anywhere] * 11,
        out_specs=vmem,
        scratch_shapes=scratch,
        compiler_params=pltpu.CompilerParams(
            collective_id=0, has_side_effects=True, vmem_limit_bytes=60 * 1024 * 1024
        ),
        name="layer",
    )(
        layer_in,
        attn_gain.reshape(1, full),
        log_decay,
        write_rate,
        head_gain.reshape(1, width),
        ffn_gain.reshape(1, full),
        qkv_weight,
        out_weight,
        gate_weight,
        up_weight,
        down_weight,
    )


def layer(shape, tp_size):
    x_size, z_size, cores = shape
    in_specs = (
        P(SEQ, "tp"),
        P(),
        P(None, None, "tp"),
        P("tp", SEQ),
        P("tp", SEQ),
        P(),
        P("tp", None),
        P(),
        P(None, "tp"),
        P(None, "tp"),
        P("tp", None),
    )
    return functools.partial(body, (x_size, z_size, tp_size)), in_specs, P(SEQ, "tp")


def solution(mesh):
    torus = Mesh(mesh.devices.reshape(4, 8, 2, mesh.shape["tp"]), (*SEQ, "tp"))
    function, in_specs, out_specs = layer((4, 8, 2), mesh.shape["tp"])
    return jax.shard_map(
        function, mesh=torus, in_specs=in_specs, out_specs=out_specs, check_vma=False
    )
```

```python
import functools

import jax
import jax.numpy as jnp
from jax import lax
from jax.experimental import pallas as pl
from jax.experimental.pallas import tpu as pltpu
from jax.sharding import Mesh
from jax.sharding import PartitionSpec as P

SEQ = ("seq_0", "seq_1", "seq_2")
MESH = pl.DeviceIdType.MESH
BF16 = jnp.bfloat16
F32 = jnp.float32

norm_floor = 0.1
head_floor = 0.05
SPAN = 128
GROUP = 2
AHEAD = 3


def mm(a, b, dims=((1,), (0,))):
    return lax.dot_general(
        a.astype(BF16), b.astype(BF16), (dims, ((), ())), preferred_element_type=F32
    )


def mm_exact(a, b):
    return lax.dot_general(
        a, b, (((1,), (0,)), ((), ())), preferred_element_type=F32, precision=lax.Precision.HIGHEST
    )


def unit_rows(vectors):
    return vectors * lax.rsqrt(jnp.sum(vectors * vectors, axis=-1, keepdims=True) + 1.0)


def iotas(size):
    rows = lax.broadcasted_iota(jnp.int32, (size, size), 0)
    cols = lax.broadcasted_iota(jnp.int32, (size, size), 1)
    return (rows, cols)


def inverses(lowers):
    size = lowers[0].shape[0]
    rows, cols = iotas(size)
    pairs = rows // 2 == cols // 2
    found = [jnp.where(rows == cols, 1.0, jnp.where(pairs, -a, 0.0)) for a in lowers]
    block = 2
    while block < size:
        wide = min(4 * block, size)
        pick = (rows // wide == cols // wide) & (rows // block != cols // block)
        inner = [mm(x, jnp.where(pick, a, 0.0)) for a, x in zip(lowers, found)]
        near = [x - mm(n, x) for n, x in zip(inner, found)]
        twice = [mm(n, n) for n in inner]
        found = [x + mm(n, x) for n, x in zip(twice, near)]
        block *= 4
    return found


def compose(earlier, later):
    first_growth, first = earlier
    second_growth, second = later
    width = first.shape[0]
    second_map = second[:, :width]
    both_growth = jnp.concatenate([second_growth, second_growth], axis=1)
    own = jnp.concatenate([first_growth * second_map, second[:, width:]], axis=1)
    return (first_growth * second_growth, both_growth * first + own - mm(second_map, first))


def apply_terms(terms, state):
    growth, both = terms
    width = both.shape[0]
    return growth * state - mm(both[:, :width], state) + both[:, width:]


def packed(terms):
    growth, both = terms
    high = growth.astype(BF16).astype(F32)
    middle = (growth - high).astype(BF16).astype(F32)
    low = growth - high - middle
    width = both.shape[0]
    row = lax.broadcasted_iota(jnp.int32, (16, width), 0)
    parts = jnp.where(row == 0, high, jnp.where(row == 1, middle, jnp.where(row == 2, low, 0.0)))
    return jnp.concatenate([both[:, :width], parts], axis=0).astype(BF16), both[:, width:].astype(BF16)


def keep(message, terms):
    upper, lower = packed(terms)
    message[0] = upper
    message[1, pl.ds(0, lower.shape[0]), :] = lower


def unpacked(message):
    width = message.shape[2]
    upper = message[0].astype(F32)
    growth = upper[width : width + 1] + upper[width + 1 : width + 2] + upper[width + 2 : width + 3]
    lower = message[1, pl.ds(0, width), :].astype(F32)
    return (growth, jnp.concatenate([upper[:width], lower], axis=1))


def choose(first, terms, others):
    return tuple(jnp.where(first, a, b) for a, b in zip(terms, others))


def ring_gather(axis, size, held, send_sem, recv_sem, arrived):
    here = lax.axis_index(axis)
    right, left = (lax.rem(here + 1, size), lax.rem(here + size - 1, size))
    width = held.shape[3]

    def copy(way, step, part):
        owner = lax.rem(here + size - step, size) if way == 0 else lax.rem(here + step, size)
        piece = held.at[owner, part, pl.ds(0, width + 16 if part == 0 else width)]
        return pltpu.make_async_remote_copy(
            src_ref=piece,
            dst_ref=piece,
            send_sem=send_sem.at[way, part, step],
            recv_sem=recv_sem.at[way, part, step],
            device_id={axis: right if way == 0 else left},
            device_id_type=MESH,
        )

    steps = size // 2
    order = ((0, 1), (1, 0))
    copies = [
        [
            {
                part: copy(way, step, part)
                for part in order[way]
                if part == way or 2 * (step + 1) < size
            }
            for step in range(steps)
        ]
        for way in (0, 1)
    ]
    for n in (0, 1):
        for way in (0, 1):
            if order[way][n] in copies[way][0]:
                copies[way][0][order[way][n]].start()
    arrived(-1, ())
    for step in range(steps):
        for n in (0, 1):
            for way in (0, 1):
                part = order[way][n]
                if part in copies[way][step]:
                    copies[way][step][part].wait_recv()
                    if step + 1 < steps and part in copies[way][step + 1]:
                        copies[way][step + 1][part].start()
        arrived(step, (0, 1) if 2 * (step + 1) < size else (0,))
    return [one for way in copies for step in way for one in step.values()]


def layer_kernel(
    sizes,
    x_hbm,
    attn_gain_hbm,
    decay_hbm,
    rate_hbm,
    head_gain_hbm,
    ffn_gain_hbm,
    qkv_hbm,
    out_hbm,
    gate_hbm,
    up_hbm,
    down_hbm,
    o_ref,
    attn_gain_ref,
    decay_ref,
    rate_ref,
    head_gain_ref,
    ffn_gain_ref,
    qkv_w,
    out_w,
    gate_w,
    up_w,
    down_w,
    rows_all,
    terms_all,
    running,
    growth_now,
    fade_of,
    system_of,
    grown_of,
    side_of,
    rate_of,
    tail_of,
    total_of,
    pair_mine,
    pair_other,
    z_held,
    x_held,
    states,
    leaving,
    parts,
    passing,
    joined,
    landed,
    resid,
    kept,
    load_sem,
    x_send,
    x_recv,
    h_send,
    h_recv,
    r_send,
    r_recv,
    w_send,
    w_recv,
    wz_send,
    wz_recv,
    wx_send,
    wx_recv,
    st_send,
    st_recv,
    pair_send,
    pair_recv,
    z_send,
    z_recv,
    s_send,
    s_recv,
):
    x_size, z_size, tp_size, blocks = sizes
    me = lax.axis_index("tp")
    core = lax.axis_index("seq_2")
    z_here = lax.axis_index("seq_1")
    x_here = lax.axis_index("seq_0")
    right, left = (lax.rem(me + 1, tp_size), lax.rem(me + tp_size - 1, tp_size))
    opposite = lax.rem(me + 2, tp_size)
    width = head_gain_ref.shape[1]
    heads = decay_ref.shape[0]
    slice_width = x_hbm.shape[1]
    shard_rows = heads * width
    half = SPAN // 2
    near = {"tp": right}, {"tp": left}

    loads = [
        pltpu.make_async_copy(qkv_hbm, qkv_w, load_sem.at[0]),
        pltpu.make_async_copy(out_hbm, out_w.at[0], load_sem.at[1]),
        pltpu.make_async_copy(gate_hbm, gate_w, load_sem.at[2]),
        pltpu.make_async_copy(up_hbm, up_w, load_sem.at[3]),
        pltpu.make_async_copy(down_hbm, down_w, load_sem.at[4]),
    ]
    early_loads = [
        pltpu.make_async_copy(source, target, load_sem.at[5 + n])
        for n, (source, target) in enumerate(
            (
                (x_hbm, rows_all.at[me]),
                (decay_hbm, decay_ref),
                (rate_hbm, rate_ref),
                (attn_gain_hbm, attn_gain_ref),
                (head_gain_hbm, head_gain_ref),
                (ffn_gain_hbm, ffn_gain_ref),
            )
        )
    ]
    for load in early_loads:
        load.start()
    barrier = pltpu.get_barrier_semaphore()
    around = (right, left, opposite)
    friends = [{"tp": other} for other in around] + [{"seq_2": 1 - core}]
    friends += [{"tp": other, "seq_2": 1 - core} for other in around]
    for axis, here, size in (("seq_1", z_here, z_size), ("seq_0", x_here, x_size)):
        friends.append({axis: lax.rem(here + 1, size)})
        friends.append({axis: lax.rem(here + size - 1, size)})
    for friend in friends:
        pl.semaphore_signal(barrier, inc=1, device_id=friend, device_id_type=MESH)
    for load in loads:
        load.start()
    early_loads[0].wait()
    pl.semaphore_wait(barrier, len(friends))

    def span_of(block, start=0, size=SPAN):
        return pl.ds(pl.multiple_of(block * SPAN + start, half), size)

    def remote(source, target, send, recv, device):
        return pltpu.make_async_remote_copy(
            src_ref=source,
            dst_ref=target,
            send_sem=send,
            recv_sem=recv,
            device_id=device,
            device_id_type=MESH,
        )

    group = GROUP * SPAN
    groups = blocks // GROUP

    def group_of(block, start=0, size=group):
        return pl.ds(pl.multiple_of(block * group + start, half), size)

    def x_first(block, way):
        there = rows_all.at[me, span_of(block)]
        return remote(there, there, x_send.at[way, block], x_recv.at[way, block], near[way])

    def x_second(block, way):
        owner = left if way == 0 else right
        there = rows_all.at[owner, span_of(block, way * half, half)]
        return remote(
            there, there, x_send.at[2 + way, block], x_recv.at[2 + way, block], near[way]
        )

    def t_first(block, way):
        there = terms_all.at[me, group_of(block)]
        return remote(there, there, h_send.at[way, block], h_recv.at[way, block], near[way])

    def t_second(block, way):
        owner = left if way == 0 else right
        there = terms_all.at[owner, group_of(block, way * group // 2, group // 2)]
        return remote(
            there, there, h_send.at[2 + way, block], h_recv.at[2 + way, block], near[way]
        )

    full = tp_size * slice_width
    core_rows = shard_rows // 2
    piece_rows = core_rows // z_size
    piece_cols = full // x_size

    def w_piece(z_at, x_at, start=0, size=piece_cols):
        first = pl.multiple_of(core * core_rows + z_at * piece_rows, piece_rows)
        return (
            pl.ds(first, piece_rows),
            pl.ds(pl.multiple_of(x_at * piece_cols + start, piece_cols // 2), size),
        )

    def w_column(x_at, start=0, size=piece_cols):
        return (
            pl.ds(pl.multiple_of(core * core_rows, core_rows), core_rows),
            pl.ds(pl.multiple_of(x_at * piece_cols + start, piece_cols // 2), size),
        )

    own_rows, own_cols = w_piece(z_here, x_here)
    w_cross = [
        remote(
            out_hbm.at[own_rows, own_cols],
            out_w.at[slot, own_rows, own_cols],
            w_send.at[n],
            w_recv.at[n],
            {"tp": other},
        )
        for n, (other, slot) in enumerate(zip(around, (2, 1, 3)))
    ]

    def w_ring(axis, here, size, region, send, recv):
        copies = []
        for step in range(size // 2):
            pair = []
            for way in (0, 1):
                owner = lax.rem(here + (size - step if way == 0 else step), size)
                last = 2 * (step + 1) == size
                half_cols = piece_cols // 2
                rows, cols = region(owner, way * half_cols, half_cols) if last else region(owner)
                there = out_w.at[pl.ds(1, tp_size - 1), rows, cols]
                onward = {axis: lax.rem(here + (1 if way == 0 else size - 1), size)}
                pair.append(remote(there, there, send.at[way, step], recv.at[way, step], onward))
            copies.append(pair)
        return copies

    w_z = w_ring(
        "seq_1", z_here, z_size, lambda at, *cut: w_piece(at, x_here, *cut), wz_send, wz_recv
    )
    w_x = w_ring("seq_0", x_here, x_size, w_column, wx_send, wx_recv)
    w_waves = [w_cross] + w_z + w_x
    half_out_w = out_w.at[pl.ds(1, tp_size - 1), pl.ds(pl.multiple_of(core * core_rows, core_rows), core_rows)]
    w_across = remote(half_out_w, half_out_w, w_send.at[3], w_recv.at[3], {"seq_2": 1 - core})

    def w_move(wave):
        for one in w_waves[wave]:
            one.wait_recv()
        for one in w_waves[wave + 1] if wave + 1 < len(w_waves) else [w_across]:
            one.start()

    def prepare(block):
        rows, cols = iotas(SPAN)
        ones = jnp.ones((SPAN, SPAN), F32)
        upper = jnp.where(rows <= cols, 1.0, 0.0)
        for h in range(heads):
            tokens = span_of(block)
            decay = jnp.broadcast_to(decay_ref[h : h + 1, tokens], (SPAN, SPAN))
            rate = jnp.broadcast_to(rate_ref[h : h + 1, tokens], (SPAN, SPAN))
            along = mm_exact(decay[0:8], upper)[0:1]
            total = mm_exact(decay[0:8], ones)[0:1]
            down = mm_exact(jnp.where(rows >= cols, decay, 0.0), ones)
            beta = mm_exact(jnp.where(rows == cols, rate, 0.0), ones)
            fade = jnp.where(rows >= cols, jnp.exp(jnp.minimum(down - along, 0.0)), 0.0)
            grown = jnp.exp(down)
            fade_of[h, tokens, :] = fade
            system_of[h, tokens, :] = jnp.where(rows > cols, beta * fade, 0.0)
            grown_of[h, tokens, :] = grown
            side_of[h, tokens, :] = beta * grown
            rate_of[h, tokens, :] = beta
            tail_of[h, tokens, :] = jnp.exp(total - down)
            total_of[h, block] = jnp.broadcast_to(jnp.exp(total), total_of.shape[2:])

    def project(block):
        tokens = group_of(block)
        spread = [rows_all[j, tokens, :].astype(F32) for j in range(tp_size)]
        squares = sum(jnp.sum(part * part, axis=1, keepdims=True) for part in spread)
        scale = lax.rsqrt(squares * (1.0 / (tp_size * slice_width)) + norm_floor)
        normed = jnp.concatenate(
            [
                (part * scale * attn_gain_ref[:, j * slice_width : (j + 1) * slice_width]).astype(
                    BF16
                )
                for j, part in enumerate(spread)
            ],
            axis=1,
        )
        return normed

    chains = [(c, h) for c in range(GROUP) for h in range(heads)]

    def cut(part):
        return [part[c * SPAN : (c + 1) * SPAN, h * width : (h + 1) * width] for c, h in chains]

    def recur(block):
        normed = project(block)
        spans = [span_of(block * GROUP + c) for c, h in chains]

        def stored(ref):
            return [ref[h, tokens, :] for (c, h), tokens in zip(chains, spans)]

        keys = [unit_rows(part) for part in cut(jnp.dot(normed, qkv_w[1], preferred_element_type=F32))]
        key_key = [mm(k, k, ((1,), (1,))) for k in keys]
        values = cut(jnp.dot(normed, qkv_w[2], preferred_element_type=F32))
        inverse = inverses([kk * f for kk, f in zip(key_key, stored(system_of))])
        sides = [
            jnp.concatenate([g * k, b * v], axis=1)
            for b, g, k, v in zip(stored(rate_of), stored(side_of), keys, values)
        ]
        solved = [mm(x, s).astype(BF16) for x, s in zip(inverse, sides)]
        tails = [k * t for k, t in zip(keys, stored(tail_of))]
        terms = [mm(k, s, ((0,), (0,))) for k, s in zip(tails, solved)]
        before = []
        for n, (c, h) in enumerate(chains):
            growth = growth_now[h][0:1]
            entry_terms = running[h]
            before.append((growth, entry_terms))
            step = total_of[h, block * GROUP + c][0:1]
            new_growth, new_terms = compose((growth, entry_terms), (step, terms[n]))
            running[h] = new_terms
            growth_now[h] = jnp.broadcast_to(new_growth, growth_now.shape[1:])
        return (block, spans, stored, normed, keys, solved, before)

    def query(known):
        block, spans, stored, normed, keys, solved, before = known
        queries = [unit_rows(part) for part in cut(jnp.dot(normed, qkv_w[0], preferred_element_type=F32))]
        query_key = [mm(q, k, ((1,), (1,))) for q, k in zip(queries, keys)]
        mixed = [mm(qk * f, s) for qk, f, s in zip(query_key, stored(fade_of), solved)]
        entries = [
            g * q - m[:, :width] for g, q, m in zip(stored(grown_of), queries, mixed)
        ]
        reached = [mm(e, b[1]) for e, b in zip(entries, before)]
        for n, ((c, h), tokens) in enumerate(zip(chains, spans)):
            local = mixed[n][:, width:] + reached[n][:, width:]
            onward = before[n][0] * entries[n] - reached[n][:, :width]
            terms_all[me, tokens, h * width : (h + 1) * width] = local.astype(BF16)
            terms_all[me, tokens, (heads + h) * width : (heads + h + 1) * width] = onward.astype(
                BF16
            )

    for block in range(min(AHEAD, blocks)):
        for way in (0, 1):
            x_first(block, way).start()
        if block == 0:
            for one in w_cross:
                one.start()
    running[...] = jnp.zeros_like(running)
    growth_now[...] = jnp.ones_like(growth_now)

    for load in early_loads[1:]:
        load.wait()

    @pl.loop(0, blocks)
    def _(block):
        prepare(block)

    loads[0].wait()
    w_move(0)

    slots = [(n, when) for n in range(groups) for when in (("early", "late") if n else ("early",))]
    plan = list(zip(range(1, len(w_waves) - 2), slots))
    early = [(wave, n) for wave, (n, when) in plan if when == "early"]
    late = [(wave, n) for wave, (n, when) in plan if when == "late"]

    @pl.loop(0, groups)
    def _(block):
        for part in range(GROUP):
            now = block * GROUP + part
            for way in (0, 1):
                x_first(now, way).wait_recv()
                x_second(now, way).start()

            @pl.when(now + AHEAD < blocks)
            def _(now=now):
                for way in (0, 1):
                    x_first(now + AHEAD, way).start()

        for wave, at in early:

            @pl.when(block == at)
            def _(wave=wave):
                w_move(wave)

        @pl.when(block > 0)
        def _():
            for part in range(GROUP):
                for way in (0, 1):
                    x_second((block - 1) * GROUP + part, way).wait_recv()
            query(recur(block - 1))

        for wave, at in late:

            @pl.when(block == at)
            def _(wave=wave):
                w_move(wave)

    for block in range(groups - 1):
        for way in (0, 1):
            t_first(block, way).start()
    for block in range(blocks - GROUP, blocks):
        for way in (0, 1):
            x_second(block, way).wait_recv()
    last = recur(groups - 1)
    w_left = len(w_waves) - 1 - len(early) - len(late)
    for wave in range(len(w_waves) - w_left, len(w_waves) - 1):
        w_move(wave)

    partner = {"seq_2": 1 - core}
    for h in range(heads):
        keep(pair_mine.at[h], (growth_now[h][0:1], running[h]))
    pair_copy = remote(pair_mine, pair_other, pair_send.at[0], pair_recv.at[0], partner)
    pair_copy.start()
    pair_copy.wait_recv()
    own, other = (unpacked(pair_mine.at[core]), unpacked(pair_other.at[core]))
    chip = compose(choose(core == 0, own, other), choose(core == 0, other, own))
    keep(z_held.at[z_here], chip)
    nothing = (jnp.ones((1, width), F32), jnp.zeros((width, 2 * width), F32))
    sums = {"before": [nothing, nothing], "after": [nothing, nothing]}

    def t_pass(block):
        for way in (0, 1):
            t_first(block, way).wait_recv()
            t_second(block, way).start()

    def z_arrived(step, ways):
        if step < 0:
            query(last)
            for way in (0, 1):
                t_first(groups - 1, way).start()
        if 0 < step < groups:
            t_pass(step - 1)
        for way in ways:
            earlier = z_here > step if way == 0 else z_here + 1 + step >= z_size
            owner = lax.rem(z_here + (z_size - 1 - step if way == 0 else 1 + step), z_size)
            item = unpacked(z_held.at[owner])
            so_far = choose(earlier, sums["before"][way], sums["after"][way])
            joint = compose(item, so_far) if way == 0 else compose(so_far, item)
            sums["before"][way] = choose(earlier, joint, sums["before"][way])
            sums["after"][way] = choose(earlier, sums["after"][way], joint)

    ring_copies = ring_gather("seq_1", z_size, z_held, z_send, z_recv, z_arrived)
    through = compose(sums["before"][1], sums["before"][0])
    rest = compose(sums["after"][1], sums["after"][0])
    keep(x_held.at[x_here], compose(compose(through, chip), rest))

    folded = []
    first_terms = choose(core == 0, own, other)

    def x_arrived(step, ways):
        if step < 0:
            w_move(len(w_waves) - 1)
            for block in range(max(0, min(groups, z_size // 2) - 1), groups - 1):
                t_pass(block)
        if step == 0:
            t_pass(groups - 1)
        if step == x_size // 2 - 2:
            older, newer = (jnp.zeros((width, width), F32), nothing)
            for back in range(x_size - 1, 0, -1):
                item = unpacked(x_held.at[lax.rem(x_here + x_size - back, x_size)])
                if back > x_size // 2:
                    older = jnp.where(x_here >= back, apply_terms(item, older), older)
                if back < x_size // 2:
                    newer = choose(x_here >= back, compose(newer, item), newer)
            folded.append((older, compose(newer, through)))
            folded.append(compose(folded[0][1], first_terms))

    ring_copies += ring_gather("seq_0", x_size, x_held, s_send, s_recv, x_arrived)
    (chosen, to_first), to_second = folded
    far = lax.rem(x_here + x_size - x_size // 2, x_size)
    chosen = jnp.where(
        x_here >= x_size // 2, apply_terms(unpacked(x_held.at[far]), chosen), chosen
    )
    leaving[0] = apply_terms(to_first, chosen).astype(BF16)
    leaving[1] = apply_terms(to_second, chosen).astype(BF16)
    states[me, core] = leaving[core]
    state_copies = []
    for n, device in enumerate(friends[:7]):
        there = core if n < 3 else 1 - core
        state_copies.append(
            remote(leaving.at[there], states.at[me, core], st_send.at[n], st_recv.at[n], device)
        )
    for n in (2, 6, 0, 1, 3, 4, 5):
        state_copies[n].start()
    for load in loads[1:]:
        load.wait()
    w_across.wait_recv()
    for block in range(groups):
        for way in (0, 1):
            t_second(block, way).wait_recv()
    for n, (origin, head) in enumerate(
        [(left, core), (right, core), (opposite, core)]
        + [(me, 1 - core)]
        + [(left, 1 - core), (right, 1 - core), (opposite, 1 - core)]
    ):
        remote(
            leaving.at[0], states.at[origin, head], st_send.at[n], st_recv.at[n], {"tp": right}
        ).wait_recv()

    def r_far(block, way):
        return remote(
            parts.at[block, opposite, pl.ds(way * half, half)],
            passing.at[way, block],
            r_send.at[way, block],
            r_recv.at[way, block],
            near[way],
        )

    def r_direct(block, way):
        target = right if way == 0 else left
        piece = pl.ds((1 - way) * half, half)
        return remote(
            parts.at[block, target, piece],
            landed.at[way, block, piece],
            r_send.at[2 + way, block],
            r_recv.at[2 + way, block],
            near[way],
        )

    def r_joined(block, way):
        return remote(
            joined.at[way, block],
            landed.at[way, block, pl.ds(way * half, half)],
            r_send.at[4 + way, block],
            r_recv.at[4 + way, block],
            near[way],
        )

    def feed_forward(block):
        outs = []
        for origin in (me, *around):
            for h in range(heads):
                local = terms_all[origin, span_of(block), h * width : (h + 1) * width]
                onward = terms_all[
                    origin, span_of(block), (heads + h) * width : (heads + h + 1) * width
                ]
                raw = local.astype(F32) + mm(onward, states[origin, h])
                level = jnp.mean(raw * raw, axis=-1, keepdims=True)
                outs.append((raw * lax.rsqrt(level + head_floor) * head_gain_ref[...]).astype(BF16))
        attended = jnp.concatenate(outs, axis=1)
        squares = jnp.zeros((SPAN, 1), F32)
        for j in range(tp_size):
            piece = rows_all[j, span_of(block), :].astype(F32) + jnp.dot(
                attended,
                out_w[:, :, j * slice_width : (j + 1) * slice_width].reshape(
                    tp_size * shard_rows, slice_width
                ),
                preferred_element_type=F32,
            )
            resid[j] = piece
            squares = squares + jnp.sum(piece * piece, axis=1, keepdims=True)
        scale = lax.rsqrt(squares * (1.0 / (tp_size * slice_width)) + norm_floor)
        normed = jnp.concatenate(
            [
                (
                    resid[j] * scale * ffn_gain_ref[:, j * slice_width : (j + 1) * slice_width]
                ).astype(BF16)
                for j in range(tp_size)
            ],
            axis=1,
        )
        kept[span_of(block), :] = resid[me]
        gate_act = jnp.dot(normed, gate_w[...], preferred_element_type=F32)
        up_act = jnp.dot(normed, up_w[...], preferred_element_type=F32)
        hidden = (jax.nn.silu(gate_act) * up_act).astype(BF16)
        for j in range(tp_size):
            parts[block, j] = jnp.dot(
                hidden,
                down_w[:, j * slice_width : (j + 1) * slice_width],
                preferred_element_type=F32,
            ).astype(BF16)

    def join(block):
        for way in (0, 1):
            r_far(block, way).wait_recv()
            target = right if way == 0 else left
            joined[way, block] = (
                passing[way, block].astype(F32)
                + parts[block, target, pl.ds(way * half, half), :].astype(F32)
            ).astype(BF16)
            r_joined(block, way).start()

    def finish(block):
        for way in (0, 1):
            r_direct(block, way).wait_recv()
            r_joined(block, way).wait_recv()
        total = kept[span_of(block), :] + parts[block, me].astype(F32)
        total = total + landed[0, block].astype(F32) + landed[1, block].astype(F32)
        o_ref[span_of(block), :] = total.astype(BF16)

    @pl.loop(0, blocks + 2)
    def _(block):
        @pl.when(block < blocks)
        def _():
            feed_forward(block)
            for way in (0, 1):
                r_far(block, way).start()
                r_direct(block, way).start()

        @pl.when((block > 0) & (block < blocks + 1))
        def _():
            join(block - 1)

        @pl.when(block > 1)
        def _():
            finish(block - 2)

    @pl.loop(0, blocks)
    def _(block):
        for way in (0, 1):
            x_first(block, way).wait_send()
            x_second(block, way).wait_send()
            r_far(block, way).wait_send()
            r_direct(block, way).wait_send()
            r_joined(block, way).wait_send()

    @pl.loop(0, groups)
    def _(block):
        for way in (0, 1):
            t_first(block, way).wait_send()
            t_second(block, way).wait_send()

    w_copies = [one for wave in w_waves for one in wave] + [w_across]
    for one in w_copies + state_copies + [pair_copy] + ring_copies:
        one.wait_send()


def body(
    sizes,
    layer_in,
    attn_gain,
    qkv_weight,
    log_decay,
    write_rate,
    head_gain,
    out_weight,
    ffn_gain,
    gate_weight,
    up_weight,
    down_weight,
):
    x_size, z_size, tp_size = sizes
    length, slice_width = layer_in.shape
    full = tp_size * slice_width
    width = head_gain.shape[0]
    heads = qkv_weight.shape[2] // width
    blocks = length // SPAN
    hidden = gate_weight.shape[1]
    shard_rows = out_weight.shape[0]

    vmem = pl.BlockSpec(memory_space=pltpu.VMEM)
    anywhere = pl.BlockSpec(memory_space=pl.ANY)
    dma = pltpu.SemaphoreType.DMA
    scratch = [
        pltpu.VMEM((1, full), F32),
        pltpu.VMEM((heads, length), F32),
        pltpu.VMEM((heads, length), F32),
        pltpu.VMEM((1, width), F32),
        pltpu.VMEM((1, full), F32),
        pltpu.VMEM(qkv_weight.shape, BF16),
        pltpu.VMEM((tp_size, shard_rows, full), BF16),
        pltpu.VMEM(gate_weight.shape, BF16),
        pltpu.VMEM(up_weight.shape, BF16),
        pltpu.VMEM(down_weight.shape, BF16),
        pltpu.VMEM((tp_size, length, slice_width), BF16),
        pltpu.VMEM((tp_size, length, 2 * heads * width), BF16),
        pltpu.VMEM((heads, width, 2 * width), F32),
        pltpu.VMEM((heads, 8, width), F32),
        *[pltpu.VMEM((heads, length, SPAN), F32) for _ in range(6)],
        pltpu.VMEM((heads, blocks, 8, width), F32),
        pltpu.VMEM((heads, 2, width + 16, width), BF16),
        pltpu.VMEM((heads, 2, width + 16, width), BF16),
        pltpu.VMEM((z_size, 2, width + 16, width), BF16),
        pltpu.VMEM((x_size, 2, width + 16, width), BF16),
        pltpu.VMEM((tp_size, heads, width, width), BF16),
        pltpu.VMEM((2, width, width), BF16),
        pltpu.VMEM((blocks, tp_size, SPAN, slice_width), BF16),
        pltpu.VMEM((2, blocks, SPAN // 2, slice_width), BF16),
        pltpu.VMEM((2, blocks, SPAN // 2, slice_width), BF16),
        pltpu.VMEM((2, blocks, SPAN, slice_width), BF16),
        pltpu.VMEM((tp_size, SPAN, slice_width), F32),
        pltpu.VMEM((length, slice_width), F32),
        dma((11,)),
        dma((4, blocks)),
        dma((4, blocks)),
        dma((4, blocks // GROUP)),
        dma((4, blocks // GROUP)),
        dma((6, blocks)),
        dma((6, blocks)),
        dma((4,)),
        dma((4,)),
        dma((2, z_size // 2)),
        dma((2, z_size // 2)),
        dma((2, x_size // 2)),
        dma((2, x_size // 2)),
        dma((7,)),
        dma((7,)),
        dma((2,)),
        dma((2,)),
        dma((2, 2, z_size)),
        dma((2, 2, z_size)),
        dma((2, 2, x_size)),
        dma((2, 2, x_size)),
    ]
    return pl.pallas_call(
        functools.partial(layer_kernel, (x_size, z_size, tp_size, blocks)),
        out_shape=pltpu.VMEM((length, slice_width), BF16),
        in_specs=[anywhere] * 11,
        out_specs=vmem,
        scratch_shapes=scratch,
        compiler_params=pltpu.CompilerParams(
            collective_id=0, has_side_effects=True, vmem_limit_bytes=60 * 1024 * 1024
        ),
        name="layer",
    )(
        layer_in,
        attn_gain.reshape(1, full),
        log_decay,
        write_rate,
        head_gain.reshape(1, width),
        ffn_gain.reshape(1, full),
        qkv_weight,
        out_weight,
        gate_weight,
        up_weight,
        down_weight,
    )


def layer(shape, tp_size):
    x_size, z_size, cores = shape
    in_specs = (
        P(SEQ, "tp"),
        P(),
        P(None, None, "tp"),
        P("tp", SEQ),
        P("tp", SEQ),
        P(),
        P("tp", None),
        P(),
        P(None, "tp"),
        P(None, "tp"),
        P("tp", None),
    )
    return functools.partial(body, (x_size, z_size, tp_size)), in_specs, P(SEQ, "tp")


def solution(mesh):
    torus = Mesh(mesh.devices.reshape(4, 8, 2, mesh.shape["tp"]), (*SEQ, "tp"))
    function, in_specs, out_specs = layer((4, 8, 2), mesh.shape["tp"])
    return jax.shard_map(
        function, mesh=torus, in_specs=in_specs, out_specs=out_specs, check_vma=False
    )
```
